256 devices in a mesh: row: 32 (over z, y), col: 8 (over x, core).
Axes of the slice: x: 4, y: 4, z: 8, core: 2. Of those that a mesh axis runs over, the one named last changes fastest.
Arguments:
- roll_embed: bfloat16 [512, 12288], P('col', 'row'), may hold values from -16 to 16
- expert_embed: bfloat16 [512, 16384], P('row', 'col'), may hold values from -16 to 16
- roll_weight: float32 [12288], P('row'), may hold values from 0.5 to 2
- expert_weight: float32 [16384], P('col'), may hold values from 0.5 to 2
Outputs:
- reward: float32 [12288], P('row')
- roll_pull: float32 [512, 12288], P('col', 'row')
- expert_pull: float32 [512, 16384], P('row', 'col')
The draws below stay inside these ranges and needn't reach their ends.
All inputs are finite; a program needn't handle non-finite values.
Results may differ from the reference program's by a relative error of at most 0.0022.
Values may be sent and summed in bfloat16 or wider, within the bound.
No kernel may reach another device: no remote copies, remote signals or barrier semaphores. Data moves between devices by JAX's collectives and lax.ppermute only.
A program may use at most 64 MiB of HBM per device.

```python
import math
import jax
import jax.numpy as jnp
from jax import lax

EMB = 512
ITERS = 3
NR = 12288
NE = 16384


def embed_draw(key, rows, cols):
    first = jax.random.fold_in(key, 11)
    values = jax.random.normal(first, (rows, cols), jnp.float32)
    return jnp.clip(values, -16.0, 16.0).astype(jnp.bfloat16)


def draw_roll_embed(key, part):
    return embed_draw(key, EMB, NR)


def draw_expert_embed(key, part):
    return embed_draw(key, EMB, NE)


def steps_of(rng, shape, cuts, low, largest):
    level = 1.0
    for dim, shards_of in cuts:
        steps = jax.random.uniform(jax.random.fold_in(jax.random.fold_in(rng, 6), dim), (shards_of,), jnp.float32, low / len(cuts), largest / len(cuts))
        level = level * jnp.repeat(jnp.exp(steps), shape[dim] // shards_of).reshape((-1,) + (1,) * (len(shape) - 1 - dim))
    return level


def setup_inputs(seed: int = 0) -> dict:
    arg_keys = jax.random.split(jax.random.key(seed), 5)
    roll_embed = draw_roll_embed(jax.random.fold_in(arg_keys[4], 71), 0)
    expert_embed = draw_expert_embed(jax.random.fold_in(arg_keys[4], 71), 0)
    roll_weight = jnp.clip(jnp.exp(math.log(2.0) - 1.3862944 * jax.random.uniform(arg_keys[2], (NR,), jnp.float32) ** steps_of(arg_keys[2], (NR,), ((0, 32),), -0.2, 0.2)), 0.5, 2.0)
    expert_weight = jnp.clip(jnp.exp(math.log(2.0) - 1.3862944 * jax.random.uniform(arg_keys[3], (NE,), jnp.float32) ** steps_of(arg_keys[3], (NE,), ((0, 8),), -0.2, 0.2)), 0.5, 2.0)
    return {"roll_embed": roll_embed, "expert_embed": expert_embed, "roll_weight": roll_weight, "expert_weight": expert_weight}


blur = 0.05


def cost_rows(xb, yf, sqx_b, sqy):
    cross = jnp.dot(xb.T, yf, precision=lax.Precision.HIGHEST)
    return (sqx_b[:, None] + sqy[None, :] - 2.0 * cross) / EMB


def reference(roll_embed, expert_embed, roll_weight, expert_weight):
    xf = roll_embed.astype(jnp.float32)
    yf = expert_embed.astype(jnp.float32)
    sqx = jnp.sum(xf * xf, 0)
    sqy = jnp.sum(yf * yf, 0)
    log_a = blur * jnp.log(roll_weight)
    log_b = blur * jnp.log(expert_weight)
    block = min(256, NR)
    nblocks = NR // block
    starts = jnp.arange(nblocks, dtype=jnp.int32) * block

    def rows_of(start):
        xb = lax.dynamic_slice_in_dim(xf, start, block, 1)
        sb = lax.dynamic_slice_in_dim(sqx, start, block, 0)
        return xb, cost_rows(xb, yf, sb, sqy)

    def row_lse(gvals):
        def one(start):
            xb, cost = rows_of(start)
            score = (gvals[None, :] - cost) / blur
            top = jnp.max(score, 1)
            return top + jnp.log(jnp.sum(jnp.exp(score - top[:, None]), 1))
        return lax.map(one, starts).reshape(NR)

    def col_lse(fvals):
        def step(carry, start):
            xb, cost = rows_of(start)
            fb = lax.dynamic_slice_in_dim(fvals, start, block, 0)
            score = (fb[:, None] - cost) / blur
            top = jnp.max(score, 0)
            total = jnp.sum(jnp.exp(score - top[None, :]), 0)
            high = jnp.maximum(carry[0], top)
            merged = carry[1] * jnp.exp(carry[0] - high) + total * jnp.exp(top - high)
            return (high, merged), None
        init = (jnp.full((NE,), -1e30, jnp.float32), jnp.zeros((NE,), jnp.float32))
        (top, total), _ = lax.scan(step, init, starts)
        return top + jnp.log(total)

    fvals = jnp.zeros((NR,), jnp.float32)
    gvals = jnp.zeros((NE,), jnp.float32)
    for step_index in range(ITERS):
        fvals = log_a - blur * row_lse(gvals)
        gvals = log_b - blur * col_lse(fvals)

    def final(carry, start):
        xb, cost = rows_of(start)
        fb = lax.dynamic_slice_in_dim(fvals, start, block, 0)
        plan = jnp.exp((fb[:, None] + gvals[None, :] - cost) / blur)
        rowmass = jnp.sum(plan, 1)
        score = (gvals[None, :] - cost) / blur
        top = jnp.max(score, 1)
        shifted = jnp.exp(score - top[:, None])
        reward_b = -jnp.sum(shifted * cost, 1) / jnp.sum(shifted, 1)
        plan_bf = plan.astype(jnp.bfloat16).astype(jnp.float32)
        pulled = jnp.dot(yf, plan_bf.T, precision=lax.Precision.HIGHEST)
        carry = carry + jnp.dot(xb, plan_bf, precision=lax.Precision.HIGHEST)
        return carry, (rowmass, reward_b, pulled)

    xsum, (rowmass, reward, pulled) = lax.scan(final, jnp.zeros((EMB, NE), jnp.float32), starts)
    rowmass = rowmass.reshape(NR)
    reward = reward.reshape(NR)
    pulled = jnp.transpose(pulled, (1, 0, 2)).reshape(EMB, NR)
    roll_pull = rowmass[None, :] * xf - pulled
    expert_pull = expert_weight[None, :] * yf - xsum
    return reward, roll_pull, expert_pull
```

```python
import functools
import math

import jax
import jax.numpy as jnp
from jax import lax
from jax.experimental import pallas as pl
from jax.experimental.pallas import tpu as pltpu
from jax.sharding import Mesh
from jax.sharding import PartitionSpec as P

ITERS = 3
BLUR = 0.05
LOG2E = 1.0 / math.log(2.0)
F32 = jnp.float32
BF16 = jnp.bfloat16
LANES = 128
STEP = 64


def cdiv(a, b):
    return -(-a // b)


def padded(n, m):
    return cdiv(n, m) * m


def log2_of(x):
    return jnp.log(x) * LOG2E


def merged(parts):
    high = jnp.max(parts, axis=0)
    return high + log2_of(jnp.sum(jnp.exp2(parts - high[None]), axis=0))


def rows_of_tiles(vec, tiles):
    return [vec[:, t * LANES : (t + 1) * LANES] for t in range(tiles)]


def to_column(lines, column_ref, tiles):
    for t in range(tiles):
        wide = jnp.broadcast_to(lines[t : t + 1, :], (LANES, LANES))
        column_ref[t * LANES : (t + 1) * LANES, :] = wide.T


def row_sweep(d_ref, column_ref, lines_ref):
    cols = d_ref.shape[0]
    chunks = cols // STEP
    tiles = d_ref.shape[1] // LANES

    def one(t, carry):
        lanes = pl.ds(pl.multiple_of(t * LANES, LANES), LANES)

        def score(c):
            at = slice(c * STEP, (c + 1) * STEP)
            return column_ref[at, :] + d_ref[at, lanes]

        top = score(0)
        for c in range(1, chunks):
            top = jnp.maximum(top, score(c))
        top = jnp.max(top, axis=0, keepdims=True)
        total = jnp.exp2(score(0) - top)
        for c in range(1, chunks):
            total = total + jnp.exp2(score(c) - top)
        total = jnp.sum(total, axis=0, keepdims=True)
        lines_ref[pl.ds(t, 1), :] = top + log2_of(total)
        return carry

    lax.fori_loop(0, tiles, one, 0)


def column_sweep(d_ref, lines, column_ref):
    cols = d_ref.shape[0]
    tiles = d_ref.shape[1] // LANES

    def one(c, carry):
        at = pl.ds(pl.multiple_of(c * STEP, STEP), STEP)

        def score(t):
            return lines[t : t + 1, :] + d_ref[at, t * LANES : (t + 1) * LANES]

        top = score(0)
        for t in range(1, tiles):
            top = jnp.maximum(top, score(t))
        top = jnp.max(top, axis=1, keepdims=True)
        total = jnp.exp2(score(0) - top)
        for t in range(1, tiles):
            total = total + jnp.exp2(score(t) - top)
        total = jnp.sum(total, axis=1, keepdims=True)
        column_ref[at, :] = jnp.broadcast_to(top + log2_of(total), (STEP, LANES))
        return carry

    lax.fori_loop(0, cols // STEP, one, 0)


def from_column(column_ref, lines_ref, tiles):
    for t in range(tiles):
        square = column_ref[t * LANES : (t + 1) * LANES, :].T
        lines_ref[t : t + 1, :] = square[0:1, :]


def setup_kernel(scale, here_ref, own_ref, other_ref, y_ref, la_ref, d_ref, sqx_ref, sqy_ref, out_ref,
                 x_ref, yc_ref, column_ref, lines_ref):
    core = here_ref[0]
    nrow, ncol = own_ref.shape[0], own_ref.shape[1]
    depth, width = own_ref.shape[2], own_ref.shape[3]
    yc_ref[...] = y_ref[...]
    for r in range(nrow):
        for c in range(ncol):
            mine = pl.multiple_of((2 * c + core) * depth, depth)
            theirs = pl.multiple_of((2 * c + 1 - core) * depth, depth)
            x_ref[pl.ds(mine, depth), r * width : (r + 1) * width] = own_ref[r, c]
            x_ref[pl.ds(theirs, depth), r * width : (r + 1) * width] = other_ref[r, c]
    tiles = x_ref.shape[1] // LANES
    sqx_ref[...] = jnp.zeros_like(sqx_ref)
    for t in range(tiles):
        part = x_ref[:, t * LANES : (t + 1) * LANES].astype(F32)
        sqx_ref[t : t + 1, :] = jnp.sum(part * part, axis=0, keepdims=True)
    ctiles = y_ref.shape[1] // LANES
    lines_ref[...] = jnp.zeros_like(lines_ref)
    for t in range(ctiles):
        part = y_ref[:, t * LANES : (t + 1) * LANES].astype(F32)
        lines_ref[t : t + 1, :] = jnp.sum(part * part, axis=0, keepdims=True)
    to_column(lines_ref[...], column_ref, ctiles)
    sqy_ref[...] = column_ref[...]
    column_ref[...] = column_ref[...] * (-0.5 * scale)
    for r in range(nrow):
        cross = lax.dot_general(
            y_ref[...], x_ref[:, r * width : (r + 1) * width], (((0,), (0,)), ((), ())),
            preferred_element_type=F32)
        d_ref[:, r * width : (r + 1) * width] = cross * scale
    lines_ref[...] = jnp.zeros_like(lines_ref)
    row_sweep(d_ref, column_ref, lines_ref)
    wtiles = width // LANES
    lines_ref[tiles : tiles + wtiles, :] = la_ref[0:wtiles, :]
    out_ref[...] = jnp.broadcast_to(lines_ref[...][None], out_ref.shape)


def row_kernel(parts_ref, lb_ref, d_ref, out_ref, column_ref, lines_ref):
    ctiles = d_ref.shape[0] // LANES
    g = lb_ref[...] - merged(parts_ref[...])
    to_column(g, column_ref, ctiles)
    lines_ref[...] = jnp.zeros_like(lines_ref)
    row_sweep(d_ref, column_ref, lines_ref)
    out_ref[...] = jnp.broadcast_to(lines_ref[...][None], out_ref.shape)


def column_kernel(parts_ref, la_ref, d_ref, f_ref, out_ref, column_ref, lines_ref):
    ctiles = d_ref.shape[0] // LANES
    f = la_ref[...] - merged(parts_ref[...])
    f_ref[...] = f
    column_sweep(d_ref, f, column_ref)
    lines_ref[...] = jnp.zeros_like(lines_ref)
    from_column(column_ref, lines_ref, ctiles)
    out_ref[...] = jnp.broadcast_to(lines_ref[...][None], out_ref.shape)


def three_pieces(v):
    high = v.astype(BF16)
    rest = v - high.astype(F32)
    mid = rest.astype(BF16)
    low = (rest - mid.astype(F32)).astype(BF16)
    return high, mid, low


def put_pieces(block_ref, at, values):
    block_ref[at] = jnp.zeros_like(block_ref[at])
    row = at[-1].start
    for n, v in enumerate(values):
        for m, piece in enumerate(three_pieces(v)):
            block_ref[at[:-1] + (slice(row + 3 * n + m, row + 3 * n + m + 1),)] = piece


def pieces_sum(block, row, n):
    return (
        block[row + 3 * n : row + 3 * n + 1].astype(F32)
        + block[row + 3 * n + 1 : row + 3 * n + 2].astype(F32)
        + block[row + 3 * n + 2 : row + 3 * n + 3].astype(F32)
    )


def plan_kernel(scale, emb, grid, here_ref, parts_ref, lb_ref, f_ref, sqx_ref, sqy_ref, d_ref, y_ref, x_ref,
                keep_ref, send_ref, sums_ref, xsum_ref, column_ref, plan_ref, ys_ref, lines_ref):
    core = here_ref[0]
    nrow, ncol, depth, width = grid
    cols, rows = d_ref.shape
    ctiles, tiles, chunks = cols // LANES, rows // LANES, cols // STEP
    g = lb_ref[...] - merged(parts_ref[...])
    to_column(g, column_ref, ctiles)
    back = 1.0 / emb
    unit = 2.0 / (emb * scale)

    def one(t, carry):
        lanes = pl.ds(pl.multiple_of(t * LANES, LANES), LANES)
        f = f_ref[pl.ds(t, 1), :]
        sq = sqx_ref[pl.ds(t, 1), :]
        mass = jnp.zeros((STEP, LANES), F32)
        paid = jnp.zeros((STEP, LANES), F32)
        for c in range(chunks):
            at = slice(c * STEP, (c + 1) * STEP)
            d = d_ref[at, lanes]
            p = jnp.exp2(column_ref[at, :] + d + f)
            plan_ref[at, lanes] = p.astype(BF16)
            mass = mass + p
            paid = paid + p * ((sq + sqy_ref[at, :]) * back - d * unit)
        lines_ref[0, pl.ds(t, 1), :] = jnp.sum(mass, axis=0, keepdims=True)
        lines_ref[1, pl.ds(t, 1), :] = jnp.sum(paid, axis=0, keepdims=True)
        return carry

    lax.fori_loop(0, tiles, one, 0)
    sums_ref[...] = jnp.zeros_like(sums_ref)
    wtiles = width // LANES
    for r in range(nrow):
        for w in range(wtiles):
            t = r * wtiles + w
            for n in range(2):
                sums_ref[r, n : n + 1, w * LANES : (w + 1) * LANES] = lines_ref[n, t : t + 1, :]
    for c in range(ncol):
        mine = pl.multiple_of((2 * c + core) * depth, depth)
        theirs = pl.multiple_of((2 * c + 1 - core) * depth, depth)
        ys_ref[c * depth : (c + 1) * depth, :] = y_ref[pl.ds(mine, depth), :]
        ys_ref[(ncol + c) * depth : (ncol + c + 1) * depth, :] = y_ref[pl.ds(theirs, depth), :]
    half = ncol * depth
    for r in range(nrow):
        part = plan_ref[:, r * width : (r + 1) * width]
        keep_ref[r] = lax.dot_general(
            ys_ref[:half, :], part, (((1,), (0,)), ((), ())), preferred_element_type=F32)
        send = lax.dot_general(
            ys_ref[half:, :], part, (((1,), (0,)), ((), ())), preferred_element_type=F32)
        send_ref[r, :half] = send.astype(BF16)
        put_pieces(send_ref, (r, slice(half, half + 16)), [sums_ref[r, n : n + 1] for n in range(2)])
    xsum = lax.dot_general(x_ref[...], plan_ref[...], (((1,), (1,)), ((), ())), preferred_element_type=F32)
    xsum_ref[...] = xsum.astype(BF16)


def pair_kernel(keep_ref, sums_ref, got_ref, out_ref):
    nrow, ncol, deep, width = out_ref.shape
    depth = deep - 16
    half = ncol * depth
    for r in range(nrow):
        extra = got_ref[r, half : half + 16]
        totals = [sums_ref[r, n : n + 1] + pieces_sum(extra, 0, n) for n in range(2)]
        for c in range(ncol):
            at = slice(c * depth, (c + 1) * depth)
            out_ref[r, c, :depth] = (keep_ref[r, at] + got_ref[r, at].astype(F32)).astype(BF16)
            put_pieces(out_ref, (r, c, slice(depth, depth + 16)), totals)


def roll_kernel(got_ref, x_ref, pull_ref, reward_ref):
    depth = x_ref.shape[0]
    total = got_ref[0].astype(F32)
    for k in range(1, got_ref.shape[0]):
        total = total + got_ref[k].astype(F32)
    mass = total[depth : depth + 1] + total[depth + 1 : depth + 2] + total[depth + 2 : depth + 3]
    paid = total[depth + 3 : depth + 4] + total[depth + 4 : depth + 5] + total[depth + 5 : depth + 6]
    reward_ref[...] = -paid / mass
    pull_ref[...] = mass * x_ref[...].astype(F32) - total[:depth]


def expert_kernel(got_ref, y_ref, b_ref, pull_ref):
    nz, ny, _, cols = got_ref.shape
    for q in range(ny):
        total = got_ref[0, q].astype(F32)
        for k in range(1, nz):
            total = total + got_ref[k, q].astype(F32)
        at = slice(q * cols, (q + 1) * cols)
        pull_ref[:, at] = b_ref[:, at] * y_ref[:, at].astype(F32) - total


def call(body, outs, scratch, *args, smem=0, limit=None):
    spec = pl.BlockSpec(memory_space=pltpu.VMEM)
    scalar = pl.BlockSpec(memory_space=pltpu.SMEM)
    return pl.pallas_call(
        body,
        out_shape=[jax.ShapeDtypeStruct(s, t) for s, t in outs],
        in_specs=[scalar] * smem + [spec] * (len(args) - smem),
        out_specs=[spec] * len(outs),
        scratch_shapes=[pltpu.VMEM(s, t) for s, t in scratch],
        compiler_params=pltpu.CompilerParams(vmem_limit_bytes=limit),
    )(*args)


def exchanged(x, axes):
    return lax.all_to_all(x, axes, split_axis=0, concat_axis=0, tiled=True)


def as_lines(v, lines):
    count = v.shape[0] // LANES
    return jnp.pad(v.reshape(count, LANES), ((0, lines - count), (0, 0)))


def swapped(x):
    return lax.ppermute(x, "core", [(0, 1), (1, 0)])


def shards(roll_embed, expert_embed, roll_weight, expert_weight):
    nz, ny, nx, nk = (lax.axis_size(a) for a in ("z", "y", "x", "core"))
    depth, width = roll_embed.shape
    thin, wide = expert_embed.shape
    emb = thin * nz * ny
    cols = wide // ny
    rows = width * ny
    scale = 2.0 * LOG2E / (emb * BLUR)
    core = lax.axis_index("core").astype(jnp.int32).reshape(1)
    quarter = lax.axis_index("y")

    y_blocks = jnp.moveaxis(expert_embed.reshape(thin, ny, cols), 1, 0)
    y_send = jnp.broadcast_to(y_blocks[None], (nz, ny, thin, cols)).reshape(nz * ny, thin, cols)
    x_send = jnp.broadcast_to(roll_embed[None], (ny * nx, depth, width))
    x_got = exchanged(x_send, ("y", "x"))
    x_other = swapped(x_got)
    y_all = exchanged(y_send, ("z", "y")).reshape(emb, cols)
    x_own = x_got.reshape(ny, nx, depth, width)
    x_other = x_other.reshape(ny, nx, depth, width)

    wtiles = width // LANES
    f_lines = padded(rows // LANES + wtiles, 8)
    g_lines = padded(cols // LANES, 8)
    la_own = as_lines(log2_of(roll_weight), 8)
    lb = as_lines(log2_of(lax.dynamic_slice_in_dim(expert_weight, quarter * cols, cols, 0)), g_lines)
    crowd = ny * nx * nk

    column = ((cols, LANES), F32)
    f_shape, g_shape = (crowd, f_lines, LANES), (nz, g_lines, LANES)
    d, sqx, sqy, out, x_all, y_all = call(
        functools.partial(setup_kernel, scale),
        [((cols, rows), F32), ((f_lines, LANES), F32), column, (f_shape, F32),
         ((emb, rows), BF16), ((emb, cols), BF16)],
        [column, ((f_lines, LANES), F32)],
        core, x_own, x_other, y_all, la_own, smem=1, limit=24 << 20)
    la = None
    for step in range(ITERS):
        if step:
            (out,) = call(row_kernel, [(f_shape, F32)], [column, ((f_lines, LANES), F32)],
                          got, lb, d, limit=12 << 20)
        got = exchanged(out, ("y", "x", "core"))
        if step == 0:
            firsts = got.reshape(ny, nx * nk, f_lines, LANES)[:, 0, rows // LANES : rows // LANES + wtiles]
            la = jnp.pad(firsts.reshape(rows // LANES, LANES), ((0, f_lines - rows // LANES), (0, 0)))
        f, out = call(column_kernel, [((f_lines, LANES), F32), (g_shape, F32)],
                      [column, ((g_lines, LANES), F32)], got, la, d, limit=12 << 20)
        got = exchanged(out, ("z",))

    grid = (ny, nx, depth, width)
    keep, send, sums, xsum = call(
        functools.partial(plan_kernel, scale, emb, grid),
        [((ny, nx * depth, width), F32), ((ny, nx * depth + 16, width), BF16), ((ny, 8, width), F32),
         ((emb, cols), BF16)],
        [column, ((cols, rows), BF16), ((emb, cols), BF16), ((2, f_lines, LANES), F32)],
        core, got, lb, f, sqx, sqy, d, y_all, x_all, smem=1, limit=32 << 20)
    xsum_got = exchanged(xsum.reshape(nz * ny, thin, cols), ("z", "y"))
    (pairs,) = call(pair_kernel, [((ny, nx, depth + 16, width), BF16)], [], keep, sums, swapped(send),
                    limit=16 << 20)
    pull_got = exchanged(pairs.reshape(ny * nx, depth + 16, width), ("y", "x"))
    (expert_pull,) = call(expert_kernel, [((thin, wide), F32)], [],
                          xsum_got.reshape(nz, ny, thin, cols), expert_embed, expert_weight.reshape(1, wide),
                          limit=8 << 20)
    roll_pull, reward = call(roll_kernel, [((depth, width), F32), ((1, width), F32)], [],
                             pull_got, roll_embed, limit=8 << 20)
    reward = reward.reshape(width)
    return (reward, roll_pull, expert_pull)


def solution(mesh):
    z, y = 8, 4
    torus = Mesh(mesh.devices.reshape(z, y, 4, 2), ("z", "y", "x", "core"))
    row, col = ("z", "y"), ("x", "core")
    return jax.shard_map(
        shards,
        mesh=torus,
        in_specs=(P(col, row), P(row, col), P(row), P(col)),
        out_specs=(P(row), P(col, row), P(row, col)),
        check_vma=False,
    )
```

```python
import functools
import math

import jax
import jax.numpy as jnp
from jax import lax
from jax.experimental import pallas as pl
from jax.experimental.pallas import tpu as pltpu
from jax.sharding import Mesh
from jax.sharding import PartitionSpec as P

ITERS = 3
BLUR = 0.05
LOG2E = 1.0 / math.log(2.0)
F32 = jnp.float32
BF16 = jnp.bfloat16
LANES = 128
STEP = 64


def cdiv(a, b):
    return -(-a // b)


def padded(n, m):
    return cdiv(n, m) * m


def log2_of(x):
    return jnp.log(x) * LOG2E


def merged(parts):
    high = jnp.max(parts, axis=0)
    return high + log2_of(jnp.sum(jnp.exp2(parts - high[None]), axis=0))


def rows_of_tiles(vec, tiles):
    return [vec[:, t * LANES : (t + 1) * LANES] for t in range(tiles)]


def to_column(lines, column_ref, tiles):
    for t in range(tiles):
        wide = jnp.broadcast_to(lines[t : t + 1, :], (LANES, LANES))
        column_ref[t * LANES : (t + 1) * LANES, :] = wide.T


def row_sweep(d_ref, column_ref, lines_ref):
    cols = d_ref.shape[0]
    chunks = cols // STEP
    tiles = d_ref.shape[1] // LANES

    def one(t, carry):
        lanes = pl.ds(pl.multiple_of(t * LANES, LANES), LANES)

        def score(c):
            at = slice(c * STEP, (c + 1) * STEP)
            return column_ref[at, :] + d_ref[at, lanes]

        top = score(0)
        for c in range(1, chunks):
            top = jnp.maximum(top, score(c))
        top = jnp.max(top, axis=0, keepdims=True)
        total = jnp.exp2(score(0) - top)
        for c in range(1, chunks):
            total = total + jnp.exp2(score(c) - top)
        total = jnp.sum(total, axis=0, keepdims=True)
        lines_ref[pl.ds(t, 1), :] = top + log2_of(total)
        return carry

    lax.fori_loop(0, tiles, one, 0, unroll=4)


def column_sweep(d_ref, lines, column_ref):
    cols = d_ref.shape[0]
    tiles = d_ref.shape[1] // LANES

    def one(c, carry):
        at = pl.ds(pl.multiple_of(c * STEP, STEP), STEP)

        def score(t):
            return lines[t : t + 1, :] + d_ref[at, t * LANES : (t + 1) * LANES]

        top = score(0)
        for t in range(1, tiles):
            top = jnp.maximum(top, score(t))
        top = jnp.max(top, axis=1, keepdims=True)
        total = jnp.exp2(score(0) - top)
        for t in range(1, tiles):
            total = total + jnp.exp2(score(t) - top)
        total = jnp.sum(total, axis=1, keepdims=True)
        column_ref[at, :] = jnp.broadcast_to(top + log2_of(total), (STEP, LANES))
        return carry

    lax.fori_loop(0, cols // STEP, one, 0, unroll=4)


def from_column(column_ref, lines_ref, tiles):
    for t in range(tiles):
        square = column_ref[t * LANES : (t + 1) * LANES, :].T
        lines_ref[t : t + 1, :] = square[0:1, :]


def setup_kernel(scale, grid, here_ref, *refs):
    nrow, ncol, depth, width = grid
    own_refs, other_refs = refs[:ncol], refs[ncol : 2 * ncol]
    y_hbm, la_ref, d_ref, sqx_ref, sqy_ref, out_ref, x_hbm, x_ref, y_ref, column_ref, lines_ref, sems = refs[2 * ncol :]
    core, across, along = here_ref[0], here_ref[1], here_ref[2]
    fetch_y = pltpu.make_async_copy(y_hbm, y_ref, sems.at[0])
    fetch_y.start()
    copies, n = [], 1
    for side, group in ((core, own_refs), (1 - core, other_refs)):
        for sx in range(ncol):
            c = lax.rem(across - sx + ncol, ncol)
            at = pl.multiple_of((2 * c + side) * depth, depth)
            for sy in range(nrow):
                r = lax.rem(along - sy + nrow, nrow)
                lanes = pl.multiple_of(r * width, LANES)
                copy = pltpu.make_async_copy(
                    group[sx].at[sy], x_ref.at[pl.ds(at, depth), pl.ds(lanes, width)], sems.at[n])
                copy.start()
                copies.append(copy)
                n += 1
    fetch_y.wait()
    ctiles = y_ref.shape[1] // LANES
    lines_ref[...] = jnp.zeros_like(lines_ref)
    for t in range(ctiles):
        part = y_ref[:, t * LANES : (t + 1) * LANES].astype(F32)
        lines_ref[t : t + 1, :] = jnp.sum(part * part, axis=0, keepdims=True)
    to_column(lines_ref[...], column_ref, ctiles)
    sqy_ref[...] = lines_ref[: sqy_ref.shape[0], :]
    column_ref[...] = column_ref[...] * (-0.5 * scale)
    for copy in copies:
        copy.wait()
    store_x = pltpu.make_async_copy(x_ref, x_hbm, sems.at[n])
    store_x.start()
    tiles = x_ref.shape[1] // LANES
    sqx_ref[...] = jnp.zeros_like(sqx_ref)
    for t in range(tiles):
        part = x_ref[:, t * LANES : (t + 1) * LANES].astype(F32)
        sqx_ref[t : t + 1, :] = jnp.sum(part * part, axis=0, keepdims=True)
    for r in range(nrow):
        cross = lax.dot_general(
            y_ref[...], x_ref[:, r * width : (r + 1) * width], (((0,), (0,)), ((), ())),
            preferred_element_type=F32)
        d_ref[:, r * width : (r + 1) * width] = cross * scale
    lines_ref[...] = jnp.zeros_like(lines_ref)
    row_sweep(d_ref, column_ref, lines_ref)
    wtiles = width // LANES
    lines_ref[tiles : tiles + wtiles, :] = la_ref[0:wtiles, :]
    out_ref[...] = jnp.broadcast_to(lines_ref[...][None], out_ref.shape)
    store_x.wait()


def row_kernel(parts_ref, lb_ref, d_ref, out_ref, column_ref, lines_ref):
    ctiles = d_ref.shape[0] // LANES
    g = lb_ref[...] - merged(parts_ref[...])
    to_column(g, column_ref, ctiles)
    lines_ref[...] = jnp.zeros_like(lines_ref)
    row_sweep(d_ref, column_ref, lines_ref)
    out_ref[...] = jnp.broadcast_to(lines_ref[...][None], out_ref.shape)


def column_kernel(parts_ref, la_ref, d_ref, f_ref, out_ref, column_ref, lines_ref):
    ctiles = d_ref.shape[0] // LANES
    f = la_ref[...] - merged(parts_ref[...])
    f_ref[...] = f
    column_sweep(d_ref, f, column_ref)
    lines_ref[...] = jnp.zeros_like(lines_ref)
    from_column(column_ref, lines_ref, ctiles)
    out_ref[...] = jnp.broadcast_to(lines_ref[...][None], out_ref.shape)


def three_pieces(v):
    high = v.astype(BF16)
    rest = v - high.astype(F32)
    mid = rest.astype(BF16)
    low = (rest - mid.astype(F32)).astype(BF16)
    return high, mid, low


def put_pieces(block_ref, at, row, values):
    block_ref[at + (slice(row, row + 16),)] = jnp.zeros((16, block_ref.shape[-1]), BF16)
    for n, v in enumerate(values):
        for m, piece in enumerate(three_pieces(v)):
            block_ref[at + (slice(row + 3 * n + m, row + 3 * n + m + 1),)] = piece


def pieces_sum(block, n):
    one, two, three = (block[3 * n + m : 3 * n + m + 1].astype(F32) for m in range(3))
    return one + two + three


def balanced(values):
    while len(values) > 1:
        half = len(values) // 2
        values = [values[k] + values[k + half] for k in range(half)]
    return values[0]


def plan_kernel(scale, emb, grid, here_ref, parts_ref, lb_ref, f_ref, sqx_ref, sqy_ref, d_ref, y_hbm, x_hbm,
                keep_hbm, send_ref, sums_ref, xsum_hbm, keep_ref, xsum_ref, column_ref, square_ref, plan_ref, y_ref, ys_ref, x_ref,
                lines_ref, sems):
    core = here_ref[0]
    nrow, ncol, depth, width = grid
    half = ncol * depth
    cols, rows = d_ref.shape
    ctiles, tiles, chunks = cols // LANES, rows // LANES, cols // STEP
    copies = [pltpu.make_async_copy(y_hbm, y_ref, sems.at[0]), pltpu.make_async_copy(x_hbm, x_ref, sems.at[1])]
    for copy in copies:
        copy.start()
    g = lb_ref[...] - merged(parts_ref[...])
    to_column(g, column_ref, ctiles)
    back = 1.0 / emb
    unit = 2.0 / (emb * scale)
    to_column(sqy_ref[...], square_ref, ctiles)

    def one(t, carry):
        lanes = pl.ds(pl.multiple_of(t * LANES, LANES), LANES)
        f = f_ref[pl.ds(t, 1), :]
        sq = sqx_ref[pl.ds(t, 1), :]
        mass = jnp.zeros((STEP, LANES), F32)
        paid = jnp.zeros((STEP, LANES), F32)
        for c in range(chunks):
            at = slice(c * STEP, (c + 1) * STEP)
            d = d_ref[at, lanes]
            p = jnp.exp2(column_ref[at, :] + d + f)
            plan_ref[at, lanes] = p.astype(BF16)
            mass = mass + p
            paid = paid + p * ((sq + square_ref[at, :]) * back - d * unit)
        lines_ref[0, pl.ds(t, 1), :] = jnp.sum(mass, axis=0, keepdims=True)
        lines_ref[1, pl.ds(t, 1), :] = jnp.sum(paid, axis=0, keepdims=True)
        return carry

    lax.fori_loop(0, tiles, one, 0, unroll=2)
    sums_ref[...] = jnp.zeros_like(sums_ref)
    wtiles = width // LANES
    for r in range(nrow):
        for w in range(wtiles):
            t = r * wtiles + w
            for n in range(2):
                sums_ref[r, n : n + 1, w * LANES : (w + 1) * LANES] = lines_ref[n, t : t + 1, :]
    for copy in copies:
        copy.wait()
    xsum = lax.dot_general(x_ref[...], plan_ref[...], (((1,), (1,)), ((), ())), preferred_element_type=F32)
    xsum_ref[...] = xsum.astype(BF16)
    copies = [pltpu.make_async_copy(xsum_ref, xsum_hbm, sems.at[2]), pltpu.make_async_copy(keep_ref, keep_hbm, sems.at[3])]
    copies[0].start()
    for c in range(ncol):
        mine = pl.multiple_of((2 * c + core) * depth, depth)
        theirs = pl.multiple_of((2 * c + 1 - core) * depth, depth)
        ys_ref[c * depth : (c + 1) * depth, :] = y_ref[pl.ds(mine, depth), :]
        ys_ref[half + c * depth : half + (c + 1) * depth, :] = y_ref[pl.ds(theirs, depth), :]
    for r in range(nrow):
        part = plan_ref[:, r * width : (r + 1) * width]
        pulled = lax.dot_general(ys_ref[...], part, (((1,), (0,)), ((), ())), preferred_element_type=F32)
        keep_ref[r] = pulled[:half].astype(BF16)
        send_ref[r, :half] = pulled[half:].astype(BF16)
        put_pieces(send_ref, (r,), half, [sums_ref[r, n : n + 1] for n in range(2)])
    copies[1].start()
    for copy in copies:
        copy.wait()


def pair_kernel(here_ref, keep_hbm, sums_ref, got_ref, *refs):
    outs, keep_ref, sems = refs[:-2], refs[-2], refs[-1]
    fetch = pltpu.make_async_copy(keep_hbm, keep_ref, sems.at[0])
    fetch.start()
    nrow, deep, width = outs[0].shape
    depth, ncol = deep - 16, len(outs)
    half = ncol * depth
    across = here_ref[1]
    fetch.wait()
    for r in range(nrow):
        extra = got_ref[r, half : half + 16]
        totals = [sums_ref[r, n : n + 1] + pieces_sum(extra, n) for n in range(2)]
        for s, out in enumerate(outs):
            c = lax.rem(across + s, ncol)
            at = pl.ds(pl.multiple_of(c * depth, depth), depth)
            out[r, :depth] = (keep_ref[r, at].astype(F32) + got_ref[r, at].astype(F32)).astype(BF16)
            put_pieces(out, (r,), depth, totals)


def across_kernel(here_ref, *refs):
    ins, outs = refs[: len(refs) // 2], refs[len(refs) // 2 :]
    nrow, deep, width = ins[0].shape
    depth = deep - 16
    along = here_ref[2]
    for s, out in enumerate(outs):
        r = lax.rem(along + s, nrow)
        out[:depth] = balanced([one[r, :depth].astype(F32) for one in ins]).astype(BF16)
        extras = [one[r, depth:deep] for one in ins]
        put_pieces(out, (), depth, [balanced([pieces_sum(extra, n) for extra in extras]) for n in range(2)])


def roll_kernel(here_ref, *refs):
    ins, (x_ref, pull_ref, reward_ref) = refs[:-3], refs[-3:]
    depth, deep = x_ref.shape[0], ins[0].shape[0]
    total = balanced([one[:depth].astype(F32) for one in ins])
    sums = [balanced([pieces_sum(one[depth:deep], n) for one in ins]) for n in range(2)]
    reward_ref[...] = -sums[1] / sums[0]
    pull_ref[...] = sums[0] * x_ref[...].astype(F32) - total


def expert_kernel(got_ref, y_ref, b_ref, pull_ref):
    nz, ny, _, cols = got_ref.shape
    for q in range(ny):
        total = got_ref[0, q].astype(F32)
        for k in range(1, nz):
            total = total + got_ref[k, q].astype(F32)
        at = slice(q * cols, (q + 1) * cols)
        pull_ref[:, at] = b_ref[:, at] * y_ref[:, at].astype(F32) - total


def call(body, outs, scratch, *args, smem=0, far=(), far_out=(), sems=0, limit=None):
    spec = pl.BlockSpec(memory_space=pltpu.VMEM)
    scalar = pl.BlockSpec(memory_space=pltpu.SMEM)
    away = pl.BlockSpec(memory_space=pltpu.HBM)
    ins = [scalar if n < smem else away if n in far else spec for n in range(len(args))]
    args = [pltpu.with_memory_space_constraint(a, pltpu.HBM) if n in far else a for n, a in enumerate(args)]
    scratches = [pltpu.VMEM(s, t) for s, t in scratch]
    if sems:
        scratches.append(pltpu.SemaphoreType.DMA((sems,)))
    return pl.pallas_call(
        body,
        out_shape=[pltpu.HBM(s, t) if n in far_out else jax.ShapeDtypeStruct(s, t) for n, (s, t) in enumerate(outs)],
        in_specs=ins,
        out_specs=[away if n in far_out else spec for n in range(len(outs))],
        scratch_shapes=scratches,
        compiler_params=pltpu.CompilerParams(vmem_limit_bytes=limit),
    )(*args)


def exchanged(x, axes):
    return lax.all_to_all(x, axes, split_axis=0, concat_axis=0, tiled=True)


def as_lines(v, lines):
    count = v.shape[0] // LANES
    return jnp.pad(v.reshape(count, LANES), ((0, lines - count), (0, 0)))


def swapped(x):
    return lax.ppermute(x, "core", [(0, 1), (1, 0)])


def shifted(x, axis, by):
    n = lax.axis_size(axis)
    return lax.ppermute(x, axis, [(i, (i + by) % n) for i in range(n)])


def shards(roll_embed, expert_embed, roll_weight, expert_weight):
    nz, ny, nx, nk = (lax.axis_size(a) for a in ("z", "y", "x", "core"))
    depth, width = roll_embed.shape
    thin, wide = expert_embed.shape
    emb = thin * nz * ny
    cols = wide // ny
    rows = width * ny
    scale = 2.0 * LOG2E / (emb * BLUR)
    grid = (ny, nx, depth, width)
    quarter = lax.axis_index("y")
    here = jnp.stack([lax.axis_index(a).astype(jnp.int32) for a in ("core", "x", "y")])

    y_blocks = jnp.moveaxis(expert_embed.reshape(thin, ny, cols), 1, 0)
    y_send = jnp.broadcast_to(y_blocks[None], (nz, ny, thin, cols)).reshape(nz * ny, thin, cols)
    y_all = exchanged(y_send, ("z", "y")).reshape(emb, cols)
    x_line = jnp.stack([roll_embed] + [shifted(roll_embed, "y", s) for s in range(1, ny)])
    x_own = [x_line] + [shifted(x_line, "x", s) for s in range(1, nx)]
    x_other = [swapped(x) for x in x_own]

    wtiles = width // LANES
    f_lines = padded(rows // LANES + wtiles, 8)
    g_lines = padded(cols // LANES, 8)
    la_own = as_lines(log2_of(roll_weight), 8)
    lb = as_lines(log2_of(lax.dynamic_slice_in_dim(expert_weight, quarter * cols, cols, 0)), g_lines)
    crowd = ny * nx * nk

    column = ((cols, LANES), F32)
    f_shape, g_shape = (crowd, f_lines, LANES), (nz, g_lines, LANES)
    ins = (here, *x_own, *x_other, y_all, la_own)
    d, sqx, sqy, out, x_all = call(
        functools.partial(setup_kernel, scale, grid),
        [((cols, rows), F32), ((f_lines, LANES), F32), ((g_lines, LANES), F32), (f_shape, F32),
         ((emb, rows), BF16)],
        [((emb, rows), BF16), ((emb, cols), BF16), column, ((f_lines, LANES), F32)],
        *ins, smem=1, far=range(1, 2 * nx + 2), far_out=(4,), sems=2 * nx * ny + 2, limit=24 << 20)
    la = None
    for step in range(ITERS):
        if step:
            (out,) = call(row_kernel, [(f_shape, F32)], [column, ((f_lines, LANES), F32)],
                          got, lb, d, limit=12 << 20)
        got = exchanged(out, ("y", "x", "core"))
        if step == 0:
            firsts = got.reshape(ny, nx * nk, f_lines, LANES)[:, 0, rows // LANES : rows // LANES + wtiles]
            la = jnp.pad(firsts.reshape(rows // LANES, LANES), ((0, f_lines - rows // LANES), (0, 0)))
        f, out = call(column_kernel, [((f_lines, LANES), F32), (g_shape, F32)],
                      [column, ((g_lines, LANES), F32)], got, la, d, limit=12 << 20)
        got = exchanged(out, ("z",))

    half = nx * depth
    keep, send, sums, xsum = call(
        functools.partial(plan_kernel, scale, emb, grid),
        [((ny, half, width), BF16), ((ny, half + 16, width), BF16), ((ny, 8, width), F32), ((emb, cols), BF16)],
        [((ny, half, width), BF16), ((emb, cols), BF16), column, column, ((cols, rows), BF16), ((emb, cols), BF16),
         ((emb, cols), BF16), ((emb, rows), BF16), ((2, f_lines, LANES), F32)],
        here, got, lb, f, sqx, sqy, d, y_all, x_all, smem=1, far=(7, 8), far_out=(0, 3), sems=4, limit=32 << 20)
    xsum_got = exchanged(xsum.reshape(nz * ny, thin, cols), ("z", "y"))
    line = ((ny, depth + 16, width), BF16)
    pairs = call(pair_kernel, [line] * nx, [((ny, half, width), BF16)], here, keep, sums, swapped(send),
                 smem=1, far=(1,), sems=1, limit=16 << 20)
    lines = [pairs[0]] + [shifted(pairs[s], "x", s) for s in range(1, nx)]
    ends = call(across_kernel, [(line[0][1:], BF16)] * ny, [], here, *lines, smem=1, limit=16 << 20)
    ends = [ends[0]] + [shifted(ends[s], "y", s) for s in range(1, ny)]
    roll_pull, reward = call(roll_kernel, [((depth, width), F32), ((1, width), F32)], [],
                             here, *ends, roll_embed, smem=1, limit=8 << 20)
    (expert_pull,) = call(expert_kernel, [((thin, wide), F32)], [],
                          xsum_got.reshape(nz, ny, thin, cols), expert_embed, expert_weight.reshape(1, wide),
                          limit=8 << 20)
    return (reward.reshape(width), roll_pull, expert_pull)


def solution(mesh):
    z, y = 8, 4
    torus = Mesh(mesh.devices.reshape(z, y, 4, 2), ("z", "y", "x", "core"))
    row, col = ("z", "y"), ("x", "core")
    return jax.shard_map(
        shards,
        mesh=torus,
        in_specs=(P(col, row), P(row, col), P(row), P(col)),
        out_specs=(P(row), P(col, row), P(row, col)),
        check_vma=False,
    )
```

```python
import functools
import math

import jax
import jax.numpy as jnp
from jax import lax
from jax.experimental import pallas as pl
from jax.experimental.pallas import tpu as pltpu
from jax.sharding import Mesh
from jax.sharding import PartitionSpec as P

ITERS = 3
BLUR = 0.05
LOG2E = 1.0 / math.log(2.0)
F32 = jnp.float32
BF16 = jnp.bfloat16
LANES = 128
STEP = 64


def cdiv(a, b):
    return -(-a // b)


def padded(n, m):
    return cdiv(n, m) * m


def log2_of(x):
    return jnp.log(x) * LOG2E


def merged(parts):
    high = jnp.max(parts, axis=0)
    return high + log2_of(jnp.sum(jnp.exp2(parts - high[None]), axis=0))


def to_column(lines, column_ref, tiles):
    for t in range(tiles):
        wide = jnp.broadcast_to(lines[t : t + 1, :], (LANES, LANES))
        column_ref[t * LANES : (t + 1) * LANES, :] = wide.T


def row_sweep(d_ref, column_ref, lines_ref):
    cols = d_ref.shape[0]
    chunks = cols // STEP
    tiles = d_ref.shape[1] // LANES

    def one(t, carry):
        lanes = pl.ds(pl.multiple_of(t * LANES, LANES), LANES)

        def score(c):
            at = slice(c * STEP, (c + 1) * STEP)
            return column_ref[at, :] + d_ref[at, lanes]

        top = score(0)
        for c in range(1, chunks):
            top = jnp.maximum(top, score(c))
        top = jnp.max(top, axis=0, keepdims=True)
        total = jnp.exp2(score(0) - top)
        for c in range(1, chunks):
            total = total + jnp.exp2(score(c) - top)
        total = jnp.sum(total, axis=0, keepdims=True)
        lines_ref[pl.ds(t, 1), :] = top + log2_of(total)
        return carry

    lax.fori_loop(0, tiles, one, 0, unroll=4)


def column_sweep(d_ref, lines, column_ref):
    cols = d_ref.shape[0]
    tiles = d_ref.shape[1] // LANES

    def one(c, carry):
        at = pl.ds(pl.multiple_of(c * STEP, STEP), STEP)

        def score(t):
            return lines[t : t + 1, :] + d_ref[at, t * LANES : (t + 1) * LANES]

        top = score(0)
        for t in range(1, tiles):
            top = jnp.maximum(top, score(t))
        top = jnp.max(top, axis=1, keepdims=True)
        total = jnp.exp2(score(0) - top)
        for t in range(1, tiles):
            total = total + jnp.exp2(score(t) - top)
        total = jnp.sum(total, axis=1, keepdims=True)
        column_ref[at, :] = jnp.broadcast_to(top + log2_of(total), (STEP, LANES))
        return carry

    lax.fori_loop(0, cols // STEP, one, 0, unroll=4)


def from_column(column_ref, lines_ref, tiles):
    for t in range(tiles):
        square = column_ref[t * LANES : (t + 1) * LANES, :].T
        lines_ref[t : t + 1, :] = square[0:1, :]


def gather_moves(nrow):
    return ((0, 0), (1, 0), (3, 0), (2, 0), (2, nrow // 2))


def setup_kernel(scale, grid, here_ref, *refs):
    nrow, ncol, depth, width = grid
    moves = gather_moves(nrow)
    own_refs, other_refs = refs[: len(moves)], refs[len(moves) : 2 * len(moves)]
    y_hbm, la_ref, d_ref, sqx_ref, sqy_ref, out_ref, x_hbm, x_ref, y_ref, column_ref, lines_ref, sems = refs[2 * len(moves) :]
    core, across, along = here_ref[0], here_ref[1], here_ref[2]
    fetch_y = pltpu.make_async_copy(y_hbm, y_ref, sems.at[0])
    fetch_y.start()
    copies, n = [], 1
    for side, group in ((core, own_refs), (1 - core, other_refs)):
        for (sx, first), ref in zip(moves, group):
            c = lax.rem(across - sx + ncol, ncol)
            at = pl.multiple_of((2 * c + side) * depth, depth)
            for k in range(ref.shape[0]):
                r = lax.rem(along - (first + k) + nrow, nrow)
                lanes = pl.multiple_of(r * width, LANES)
                copy = pltpu.make_async_copy(
                    ref.at[k], x_ref.at[pl.ds(at, depth), pl.ds(lanes, width)], sems.at[n])
                copy.start()
                copies.append(copy)
                n += 1
    fetch_y.wait()
    ctiles = y_ref.shape[1] // LANES
    lines_ref[...] = jnp.zeros_like(lines_ref)
    for t in range(ctiles):
        part = y_ref[:, t * LANES : (t + 1) * LANES].astype(F32)
        lines_ref[t : t + 1, :] = jnp.sum(part * part, axis=0, keepdims=True)
    to_column(lines_ref[...], column_ref, ctiles)
    sqy_ref[...] = lines_ref[: sqy_ref.shape[0], :]
    column_ref[...] = column_ref[...] * (-0.5 * scale)
    for copy in copies:
        copy.wait()
    store_x = pltpu.make_async_copy(x_ref, x_hbm, sems.at[n])
    store_x.start()
    tiles = x_ref.shape[1] // LANES
    sqx_ref[...] = jnp.zeros_like(sqx_ref)
    for t in range(tiles):
        part = x_ref[:, t * LANES : (t + 1) * LANES].astype(F32)
        sqx_ref[t : t + 1, :] = jnp.sum(part * part, axis=0, keepdims=True)
    for r in range(nrow):
        cross = lax.dot_general(
            y_ref[...], x_ref[:, r * width : (r + 1) * width], (((0,), (0,)), ((), ())),
            preferred_element_type=F32)
        d_ref[:, r * width : (r + 1) * width] = cross * scale
    lines_ref[...] = jnp.zeros_like(lines_ref)
    row_sweep(d_ref, column_ref, lines_ref)
    wtiles = width // LANES
    lines_ref[tiles : tiles + wtiles, :] = la_ref[0:wtiles, :]
    out_ref[...] = jnp.broadcast_to(lines_ref[...][None], out_ref.shape)
    store_x.wait()


def row_kernel(parts_ref, lb_ref, d_ref, out_ref, column_ref, lines_ref):
    ctiles = d_ref.shape[0] // LANES
    g = lb_ref[...] - merged(parts_ref[...])
    to_column(g, column_ref, ctiles)
    lines_ref[...] = jnp.zeros_like(lines_ref)
    row_sweep(d_ref, column_ref, lines_ref)
    out_ref[...] = jnp.broadcast_to(lines_ref[...][None], out_ref.shape)


def column_kernel(parts_ref, la_ref, d_ref, f_ref, out_ref, column_ref, lines_ref):
    ctiles = d_ref.shape[0] // LANES
    f = la_ref[...] - merged(parts_ref[...])
    f_ref[...] = f
    column_sweep(d_ref, f, column_ref)
    lines_ref[...] = jnp.zeros_like(lines_ref)
    from_column(column_ref, lines_ref, ctiles)
    out_ref[...] = jnp.broadcast_to(lines_ref[...][None], out_ref.shape)


def three_pieces(v):
    high = v.astype(BF16)
    rest = v - high.astype(F32)
    mid = rest.astype(BF16)
    low = (rest - mid.astype(F32)).astype(BF16)
    return high, mid, low


def put_pieces(block_ref, at, row, values):
    block_ref[at + (slice(row, row + 16),)] = jnp.zeros((16, block_ref.shape[-1]), BF16)
    for n, v in enumerate(values):
        for m, piece in enumerate(three_pieces(v)):
            block_ref[at + (slice(row + 3 * n + m, row + 3 * n + m + 1),)] = piece


def pieces_sum(block, n):
    one, two, three = (block[3 * n + m : 3 * n + m + 1].astype(F32) for m in range(3))
    return one + two + three


def balanced(values):
    while len(values) > 1:
        half = len(values) // 2
        values = [values[k] + values[k + half] for k in range(half)]
    return values[0]


def plan_kernel(scale, emb, grid, here_ref, parts_ref, lb_ref, f_ref, sqx_ref, sqy_ref, d_ref, y_hbm, x_hbm,
                keep_hbm, send_ref, sums_ref, xsum_hbm, keep_ref, xsum_ref, column_ref, square_ref, plan_ref, y_ref, ys_ref, x_ref,
                lines_ref, sems):
    core = here_ref[0]
    nrow, ncol, depth, width = grid
    half = ncol * depth
    cols, rows = d_ref.shape
    ctiles, tiles, chunks = cols // LANES, rows // LANES, cols // STEP
    copies = [pltpu.make_async_copy(y_hbm, y_ref, sems.at[0]), pltpu.make_async_copy(x_hbm, x_ref, sems.at[1])]
    for copy in copies:
        copy.start()
    g = lb_ref[...] - merged(parts_ref[...])
    to_column(g, column_ref, ctiles)
    back = 1.0 / emb
    unit = 2.0 / (emb * scale)
    to_column(sqy_ref[...], square_ref, ctiles)

    def one(t, carry):
        lanes = pl.ds(pl.multiple_of(t * LANES, LANES), LANES)
        f = f_ref[pl.ds(t, 1), :]
        sq = sqx_ref[pl.ds(t, 1), :]
        mass = jnp.zeros((STEP, LANES), F32)
        paid = jnp.zeros((STEP, LANES), F32)
        for c in range(chunks):
            at = slice(c * STEP, (c + 1) * STEP)
            d = d_ref[at, lanes]
            p = jnp.exp2(column_ref[at, :] + d + f)
            plan_ref[at, lanes] = p.astype(BF16)
            mass = mass + p
            paid = paid + p * ((sq + square_ref[at, :]) * back - d * unit)
        lines_ref[0, pl.ds(t, 1), :] = jnp.sum(mass, axis=0, keepdims=True)
        lines_ref[1, pl.ds(t, 1), :] = jnp.sum(paid, axis=0, keepdims=True)
        return carry

    lax.fori_loop(0, tiles, one, 0, unroll=2)
    sums_ref[...] = jnp.zeros_like(sums_ref)
    wtiles = width // LANES
    for r in range(nrow):
        for w in range(wtiles):
            t = r * wtiles + w
            for n in range(2):
                sums_ref[r, n : n + 1, w * LANES : (w + 1) * LANES] = lines_ref[n, t : t + 1, :]
    for copy in copies:
        copy.wait()
    xsum = lax.dot_general(x_ref[...], plan_ref[...], (((1,), (1,)), ((), ())), preferred_element_type=F32)
    xsum_ref[...] = xsum.astype(BF16)
    copies = [pltpu.make_async_copy(xsum_ref, xsum_hbm, sems.at[2]), pltpu.make_async_copy(keep_ref, keep_hbm, sems.at[3])]
    copies[0].start()
    for c in range(ncol):
        mine = pl.multiple_of((2 * c + core) * depth, depth)
        theirs = pl.multiple_of((2 * c + 1 - core) * depth, depth)
        ys_ref[c * depth : (c + 1) * depth, :] = y_ref[pl.ds(mine, depth), :]
        ys_ref[half + c * depth : half + (c + 1) * depth, :] = y_ref[pl.ds(theirs, depth), :]
    for r in range(nrow):
        part = plan_ref[:, r * width : (r + 1) * width]
        pulled = lax.dot_general(ys_ref[...], part, (((1,), (0,)), ((), ())), preferred_element_type=F32)
        keep_ref[r] = pulled[:half].astype(BF16)
        send_ref[r, :half] = pulled[half:].astype(BF16)
        put_pieces(send_ref, (r,), half, [sums_ref[r, n : n + 1] for n in range(2)])
    copies[1].start()
    for copy in copies:
        copy.wait()


def pair_kernel(here_ref, keep_hbm, sums_ref, got_ref, *refs):
    outs, keep_ref, sems = refs[:-2], refs[-2], refs[-1]
    fetch = pltpu.make_async_copy(keep_hbm, keep_ref, sems.at[0])
    fetch.start()
    nrow, deep, _ = outs[0].shape
    half = keep_ref.shape[1]
    depth = deep - 16
    ncol = half // depth
    across = here_ref[1]
    totals = []
    for r in range(nrow):
        extra = got_ref[r, half : half + 16]
        totals.append([sums_ref[r, n : n + 1] + pieces_sum(extra, n) for n in range(2)])
    fetch.wait()
    for (s, first), out in zip(gather_moves(nrow), outs):
        c = lax.rem(across + s, ncol)
        at = pl.ds(pl.multiple_of(c * depth, depth), depth)
        for k in range(out.shape[0]):
            r = first + k
            out[k, :depth] = (keep_ref[r, at].astype(F32) + got_ref[r, at].astype(F32)).astype(BF16)
            put_pieces(out, (k,), depth, totals[r])


def across_kernel(here_ref, *refs):
    moves = gather_moves(refs[0].shape[0])
    ins, outs = refs[: len(moves)], refs[len(moves) : 2 * len(moves) - 1]
    total_ref, extra_ref = refs[2 * len(moves) - 1 :]
    nrow, deep, _ = ins[0].shape
    depth = deep - 16
    along = here_ref[2]
    for r in range(nrow):
        ends = [ins[0][r], ins[1][r], ins[3 + 2 * r // nrow][r % (nrow // 2)], ins[2][r]]
        total_ref[r] = balanced([one[:depth].astype(F32) for one in ends])
        for n in range(2):
            extra_ref[r, n : n + 1] = balanced([pieces_sum(one[depth:deep], n) for one in ends])
    for s, out in enumerate(outs):
        r = lax.rem(along + s, nrow)
        out[:depth] = total_ref[r].astype(BF16)
        put_pieces(out, (), depth, [extra_ref[r, n : n + 1] for n in range(2)])


def roll_kernel(here_ref, *refs):
    ins, (x_ref, pull_ref, reward_ref) = refs[:-3], refs[-3:]
    depth, deep = x_ref.shape[0], ins[0].shape[0]
    total = balanced([one[:depth].astype(F32) for one in ins])
    sums = [balanced([pieces_sum(one[depth:deep], n) for one in ins]) for n in range(2)]
    reward_ref[...] = -sums[1] / sums[0]
    pull_ref[...] = sums[0] * x_ref[...].astype(F32) - total


def expert_kernel(got_ref, y_ref, b_ref, pull_ref):
    nz, ny, _, cols = got_ref.shape
    for q in range(ny):
        total = got_ref[0, q].astype(F32)
        for k in range(1, nz):
            total = total + got_ref[k, q].astype(F32)
        at = slice(q * cols, (q + 1) * cols)
        pull_ref[:, at] = b_ref[:, at] * y_ref[:, at].astype(F32) - total


def call(body, outs, scratch, *args, smem=0, far=(), far_out=(), sems=0, limit=None):
    spec = pl.BlockSpec(memory_space=pltpu.VMEM)
    scalar = pl.BlockSpec(memory_space=pltpu.SMEM)
    away = pl.BlockSpec(memory_space=pltpu.HBM)
    ins = [scalar if n < smem else away if n in far else spec for n in range(len(args))]
    args = [pltpu.with_memory_space_constraint(a, pltpu.HBM) if n in far else a for n, a in enumerate(args)]
    scratches = [pltpu.VMEM(s, t) for s, t in scratch]
    if sems:
        scratches.append(pltpu.SemaphoreType.DMA((sems,)))
    return pl.pallas_call(
        body,
        out_shape=[pltpu.HBM(s, t) if n in far_out else jax.ShapeDtypeStruct(s, t) for n, (s, t) in enumerate(outs)],
        in_specs=ins,
        out_specs=[away if n in far_out else spec for n in range(len(outs))],
        scratch_shapes=scratches,
        compiler_params=pltpu.CompilerParams(vmem_limit_bytes=limit),
    )(*args)


def exchanged(x, axes):
    return lax.all_to_all(x, axes, split_axis=0, concat_axis=0, tiled=True)


def as_lines(v, lines):
    count = v.shape[0] // LANES
    return jnp.pad(v.reshape(count, LANES), ((0, lines - count), (0, 0)))


def swapped(x):
    return lax.ppermute(x, "core", [(0, 1), (1, 0)])


def shifted(x, axis, by):
    n = lax.axis_size(axis)
    return lax.ppermute(x, axis, [(i, (i + by) % n) for i in range(n)])


def shards(roll_embed, expert_embed, roll_weight, expert_weight):
    nz, ny, nx, nk = (lax.axis_size(a) for a in ("z", "y", "x", "core"))
    depth, width = roll_embed.shape
    thin, wide = expert_embed.shape
    emb = thin * nz * ny
    cols = wide // ny
    rows = width * ny
    scale = 2.0 * LOG2E / (emb * BLUR)
    grid = (ny, nx, depth, width)
    quarter = lax.axis_index("y")
    here = jnp.stack([lax.axis_index(a).astype(jnp.int32) for a in ("core", "x", "y")])

    x_line = [roll_embed] + [shifted(roll_embed, "y", s) for s in range(1, ny)]
    y_blocks = jnp.moveaxis(expert_embed.reshape(thin, ny, cols), 1, 0)
    y_send = jnp.broadcast_to(y_blocks[None], (nz, ny, thin, cols)).reshape(nz * ny, thin, cols)
    y_all = exchanged(y_send, ("z", "y"))
    y_all = y_all.reshape(emb, cols)
    middle = ny // 2
    x_line = jnp.stack(x_line)
    behind, ahead = shifted(x_line, "x", 1), shifted(x_line, "x", -1)
    x_own = [x_line, behind, ahead, shifted(behind[:middle], "x", 1), shifted(ahead[middle:], "x", -1)]
    x_other = [swapped(x) for x in x_own]

    wtiles = width // LANES
    f_lines = padded(rows // LANES + wtiles, 8)
    g_lines = padded(cols // LANES, 8)
    la_own = as_lines(log2_of(roll_weight), 8)
    lb = as_lines(log2_of(lax.dynamic_slice_in_dim(expert_weight, quarter * cols, cols, 0)), g_lines)
    crowd = ny * nx * nk

    column = ((cols, LANES), F32)
    f_shape, g_shape = (crowd, f_lines, LANES), (nz, g_lines, LANES)
    ins = (here, *x_own, *x_other, y_all, la_own)
    d, sqx, sqy, out, x_all = call(
        functools.partial(setup_kernel, scale, grid),
        [((cols, rows), F32), ((f_lines, LANES), F32), ((g_lines, LANES), F32), (f_shape, F32),
         ((emb, rows), BF16)],
        [((emb, rows), BF16), ((emb, cols), BF16), column, ((f_lines, LANES), F32)],
        *ins, smem=1, far=range(1, 12), far_out=(4,), sems=2 * nx * ny + 2, limit=24 << 20)
    la = None
    for step in range(ITERS):
        if step:
            (out,) = call(row_kernel, [(f_shape, F32)], [column, ((f_lines, LANES), F32)],
                          got, lb, d, limit=12 << 20)
        got = exchanged(out, ("y", "x", "core"))
        if step == 0:
            firsts = got.reshape(ny, nx * nk, f_lines, LANES)[:, 0, rows // LANES : rows // LANES + wtiles]
            la = jnp.pad(firsts.reshape(rows // LANES, LANES), ((0, f_lines - rows // LANES), (0, 0)))
        f, out = call(column_kernel, [((f_lines, LANES), F32), (g_shape, F32)],
                      [column, ((g_lines, LANES), F32)], got, la, d, limit=12 << 20)
        got = exchanged(out, ("z",))

    half = nx * depth
    keep, send, sums, xsum = call(
        functools.partial(plan_kernel, scale, emb, grid),
        [((ny, half, width), BF16), ((ny, half + 16, width), BF16), ((ny, 8, width), F32), ((emb, cols), BF16)],
        [((ny, half, width), BF16), ((emb, cols), BF16), column, column, ((cols, rows), BF16), ((emb, cols), BF16),
         ((emb, cols), BF16), ((emb, rows), BF16), ((2, f_lines, LANES), F32)],
        here, got, lb, f, sqx, sqy, d, y_all, x_all, smem=1, far=(7, 8), far_out=(0, 3), sems=4, limit=32 << 20)
    xsum_got = exchanged(xsum.reshape(nz * ny, thin, cols), ("z", "y"))
    line = ((ny, depth + 16, width), BF16)
    short = ((middle, depth + 16, width), BF16)
    own, one, three, two, other_two = call(
        pair_kernel, [line] * 3 + [short] * 2, [((ny, half, width), BF16)], here, keep, sums, swapped(send),
        smem=1, far=(1,), sems=1, limit=16 << 20)
    two, other_two = shifted(two, "x", 1), shifted(other_two, "x", -1)
    lines = [own, shifted(one, "x", 1), shifted(three, "x", -1), shifted(two, "x", 1), shifted(other_two, "x", -1)]
    ends = call(across_kernel, [(line[0][1:], BF16)] * ny, [((ny, depth, width), F32), ((ny, 8, width), F32)],
                here, *lines, smem=1, limit=16 << 20)
    ends = [ends[0]] + [shifted(ends[s], "y", s) for s in range(1, ny)]
    roll_pull, reward = call(roll_kernel, [((depth, width), F32), ((1, width), F32)], [],
                             here, *ends, roll_embed, smem=1, limit=8 << 20)
    (expert_pull,) = call(expert_kernel, [((thin, wide), F32)], [],
                          xsum_got.reshape(nz, ny, thin, cols), expert_embed, expert_weight.reshape(1, wide),
                          limit=8 << 20)
    return (reward.reshape(width), roll_pull, expert_pull)


def solution(mesh):
    z, y = 8, 4
    torus = Mesh(mesh.devices.reshape(z, y, 4, 2), ("z", "y", "x", "core"))
    row, col = ("z", "y"), ("x", "core")

    return jax.shard_map(
        shards,
        mesh=torus,
        in_specs=(P(col, row), P(row, col), P(row), P(col)),
        out_specs=(P(row), P(col, row), P(row, col)),
        check_vma=False,
    )
```

```python
import functools
import math

import jax
import jax.numpy as jnp
from jax import lax
from jax.experimental import pallas as pl
from jax.experimental.pallas import tpu as pltpu
from jax.sharding import Mesh
from jax.sharding import PartitionSpec as P

ITERS = 3
BLUR = 0.05
LOG2E = 1.0 / math.log(2.0)
F32 = jnp.float32
BF16 = jnp.bfloat16
LANES = 128
STEP = 64


def cdiv(a, b):
    return -(-a // b)


def padded(n, m):
    return cdiv(n, m) * m


def log2_of(x):
    return jnp.log(x) * LOG2E


def merged(parts):
    high = jnp.max(parts, axis=0)
    return high + log2_of(jnp.sum(jnp.exp2(parts - high[None]), axis=0))


def to_column(lines, column_ref, tiles):
    for t in range(tiles):
        wide = jnp.broadcast_to(lines[t : t + 1, :], (LANES, LANES))
        column_ref[t * LANES : (t + 1) * LANES, :] = wide.T


def row_sweep(d_ref, column_ref, lines_ref):
    cols = d_ref.shape[0]
    chunks = cols // STEP
    tiles = d_ref.shape[1] // LANES

    def one(t, carry):
        lanes = pl.ds(pl.multiple_of(t * LANES, LANES), LANES)

        def score(c):
            at = slice(c * STEP, (c + 1) * STEP)
            return column_ref[at, :] + d_ref[at, lanes]

        top = score(0)
        for c in range(1, chunks):
            top = jnp.maximum(top, score(c))
        top = jnp.max(top, axis=0, keepdims=True)
        total = jnp.exp2(score(0) - top)
        for c in range(1, chunks):
            total = total + jnp.exp2(score(c) - top)
        total = jnp.sum(total, axis=0, keepdims=True)
        lines_ref[pl.ds(t, 1), :] = top + log2_of(total)
        return carry

    lax.fori_loop(0, tiles, one, 0, unroll=4)


def column_sweep(d_ref, lines, column_ref):
    cols = d_ref.shape[0]
    tiles = d_ref.shape[1] // LANES

    def one(c, carry):
        at = pl.ds(pl.multiple_of(c * STEP, STEP), STEP)

        def score(t):
            return lines[t : t + 1, :] + d_ref[at, t * LANES : (t + 1) * LANES]

        top = score(0)
        for t in range(1, tiles):
            top = jnp.maximum(top, score(t))
        top = jnp.max(top, axis=1, keepdims=True)
        total = jnp.exp2(score(0) - top)
        for t in range(1, tiles):
            total = total + jnp.exp2(score(t) - top)
        total = jnp.sum(total, axis=1, keepdims=True)
        column_ref[at, :] = jnp.broadcast_to(top + log2_of(total), (STEP, LANES))
        return carry

    lax.fori_loop(0, cols // STEP, one, 0, unroll=4)


def from_column(column_ref, lines_ref, tiles):
    for t in range(tiles):
        square = column_ref[t * LANES : (t + 1) * LANES, :].T
        lines_ref[t : t + 1, :] = square[0:1, :]


def gather_moves(nrow):
    return ((0, 0), (1, 0), (3, 0), (2, 0), (2, nrow // 2))


def setup_kernel(scale, grid, here_ref, *refs):
    nrow, ncol, depth, width = grid
    moves = gather_moves(nrow)
    own_refs, other_refs = refs[: len(moves)], refs[len(moves) : 2 * len(moves)]
    y_hbm, la_ref, d_ref, sqx_ref, sqy_ref, out_ref, x_hbm, x_ref, y_ref, column_ref, lines_ref, sems = refs[2 * len(moves) :]
    core, across, along = here_ref[0], here_ref[1], here_ref[2]
    fetch_y = pltpu.make_async_copy(y_hbm, y_ref, sems.at[0])
    fetch_y.start()
    copies, n = [], 1
    for side, group in ((core, own_refs), (1 - core, other_refs)):
        for (sx, first), ref in zip(moves, group):
            c = lax.rem(across - sx + ncol, ncol)
            at = pl.multiple_of((2 * c + side) * depth, depth)
            for k in range(ref.shape[0]):
                r = lax.rem(along - (first + k) + nrow, nrow)
                lanes = pl.multiple_of(r * width, LANES)
                copy = pltpu.make_async_copy(
                    ref.at[k], x_ref.at[pl.ds(at, depth), pl.ds(lanes, width)], sems.at[n])
                copy.start()
                copies.append(copy)
                n += 1
    fetch_y.wait()
    ctiles = y_ref.shape[1] // LANES
    lines_ref[...] = jnp.zeros_like(lines_ref)
    for t in range(ctiles):
        part = y_ref[:, t * LANES : (t + 1) * LANES].astype(F32)
        lines_ref[t : t + 1, :] = jnp.sum(part * part, axis=0, keepdims=True)
    to_column(lines_ref[...], column_ref, ctiles)
    sqy_ref[...] = lines_ref[: sqy_ref.shape[0], :]
    column_ref[...] = column_ref[...] * (-0.5 * scale)
    for copy in copies:
        copy.wait()
    store_x = pltpu.make_async_copy(x_ref, x_hbm, sems.at[n])
    store_x.start()
    tiles = x_ref.shape[1] // LANES
    sqx_ref[...] = jnp.zeros_like(sqx_ref)
    for t in range(tiles):
        part = x_ref[:, t * LANES : (t + 1) * LANES].astype(F32)
        sqx_ref[t : t + 1, :] = jnp.sum(part * part, axis=0, keepdims=True)
    for r in range(nrow):
        cross = lax.dot_general(
            y_ref[...], x_ref[:, r * width : (r + 1) * width], (((0,), (0,)), ((), ())),
            preferred_element_type=F32)
        d_ref[:, r * width : (r + 1) * width] = cross * scale
    lines_ref[...] = jnp.zeros_like(lines_ref)
    row_sweep(d_ref, column_ref, lines_ref)
    wtiles = width // LANES
    lines_ref[tiles : tiles + wtiles, :] = la_ref[0:wtiles, :]
    out_ref[...] = jnp.broadcast_to(lines_ref[...][None], out_ref.shape)
    store_x.wait()


def row_kernel(parts_ref, lb_ref, d_ref, out_ref, column_ref, lines_ref):
    ctiles = d_ref.shape[0] // LANES
    g = lb_ref[...] - merged(parts_ref[...])
    to_column(g, column_ref, ctiles)
    lines_ref[...] = jnp.zeros_like(lines_ref)
    row_sweep(d_ref, column_ref, lines_ref)
    out_ref[...] = jnp.broadcast_to(lines_ref[...][None], out_ref.shape)


def column_kernel(parts_ref, la_ref, d_ref, f_ref, out_ref, column_ref, lines_ref):
    ctiles = d_ref.shape[0] // LANES
    f = la_ref[...] - merged(parts_ref[...])
    f_ref[...] = f
    column_sweep(d_ref, f, column_ref)
    lines_ref[...] = jnp.zeros_like(lines_ref)
    from_column(column_ref, lines_ref, ctiles)
    out_ref[...] = jnp.broadcast_to(lines_ref[...][None], out_ref.shape)


def three_pieces(v):
    high = v.astype(BF16)
    rest = v - high.astype(F32)
    mid = rest.astype(BF16)
    low = (rest - mid.astype(F32)).astype(BF16)
    return high, mid, low


def put_pieces(block_ref, at, row, values):
    block_ref[at + (slice(row, row + 16),)] = jnp.zeros((16, block_ref.shape[-1]), BF16)
    for n, v in enumerate(values):
        for m, piece in enumerate(three_pieces(v)):
            block_ref[at + (slice(row + 3 * n + m, row + 3 * n + m + 1),)] = piece


def pieces_sum(block, n):
    one, two, three = (block[3 * n + m : 3 * n + m + 1].astype(F32) for m in range(3))
    return one + two + three


def balanced(values):
    while len(values) > 1:
        half = len(values) // 2
        values = [values[k] + values[k + half] for k in range(half)]
    return values[0]


def plan_kernel(scale, emb, grid, here_ref, parts_ref, lb_ref, f_ref, sqx_ref, sqy_ref, d_ref, y_hbm, x_hbm,
                keep_hbm, send_ref, sums_ref, xsum_hbm, keep_ref, xsum_ref, column_ref, square_ref, plan_ref, y_ref, ys_ref, x_ref,
                lines_ref, sems):
    core = here_ref[0]
    nrow, ncol, depth, width = grid
    half = ncol * depth
    cols, rows = d_ref.shape
    ctiles, tiles, chunks = cols // LANES, rows // LANES, cols // STEP
    copies = [pltpu.make_async_copy(y_hbm, y_ref, sems.at[0]), pltpu.make_async_copy(x_hbm, x_ref, sems.at[1])]
    for copy in copies:
        copy.start()
    g = lb_ref[...] - merged(parts_ref[...])
    to_column(g, column_ref, ctiles)
    back = 1.0 / emb
    unit = 2.0 / (emb * scale)
    to_column(sqy_ref[...], square_ref, ctiles)

    def one(t, carry):
        lanes = pl.ds(pl.multiple_of(t * LANES, LANES), LANES)
        f = f_ref[pl.ds(t, 1), :]
        sq = sqx_ref[pl.ds(t, 1), :]
        mass = jnp.zeros((STEP, LANES), F32)
        paid = jnp.zeros((STEP, LANES), F32)
        for c in range(chunks):
            at = slice(c * STEP, (c + 1) * STEP)
            d = d_ref[at, lanes]
            p = jnp.exp2(column_ref[at, :] + d + f)
            plan_ref[at, lanes] = p.astype(BF16)
            mass = mass + p
            paid = paid + p * ((sq + square_ref[at, :]) * back - d * unit)
        lines_ref[0, pl.ds(t, 1), :] = jnp.sum(mass, axis=0, keepdims=True)
        lines_ref[1, pl.ds(t, 1), :] = jnp.sum(paid, axis=0, keepdims=True)
        return carry

    lax.fori_loop(0, tiles, one, 0, unroll=2)
    sums_ref[...] = jnp.zeros_like(sums_ref)
    wtiles = width // LANES
    for r in range(nrow):
        for w in range(wtiles):
            t = r * wtiles + w
            for n in range(2):
                sums_ref[r, n : n + 1, w * LANES : (w + 1) * LANES] = lines_ref[n, t : t + 1, :]
    for copy in copies:
        copy.wait()
    xsum = lax.dot_general(x_ref[...], plan_ref[...], (((1,), (1,)), ((), ())), preferred_element_type=F32)
    xsum_ref[...] = xsum.astype(BF16)
    copies = [pltpu.make_async_copy(xsum_ref, xsum_hbm, sems.at[2]), pltpu.make_async_copy(keep_ref, keep_hbm, sems.at[3])]
    copies[0].start()
    for c in range(ncol):
        mine = pl.multiple_of((2 * c + core) * depth, depth)
        theirs = pl.multiple_of((2 * c + 1 - core) * depth, depth)
        ys_ref[c * depth : (c + 1) * depth, :] = y_ref[pl.ds(mine, depth), :]
        ys_ref[half + c * depth : half + (c + 1) * depth, :] = y_ref[pl.ds(theirs, depth), :]
    for r in range(nrow):
        part = plan_ref[:, r * width : (r + 1) * width]
        pulled = lax.dot_general(ys_ref[...], part, (((1,), (0,)), ((), ())), preferred_element_type=F32)
        keep_ref[r] = pulled[:half].astype(BF16)
        send_ref[r, :half] = pulled[half:].astype(BF16)
        put_pieces(send_ref, (r,), half, [sums_ref[r, n : n + 1] for n in range(2)])
    copies[1].start()
    for copy in copies:
        copy.wait()


def pair_kernel(here_ref, keep_hbm, sums_ref, got_ref, *refs):
    outs, keep_ref, sems = refs[:-2], refs[-2], refs[-1]
    fetch = pltpu.make_async_copy(keep_hbm, keep_ref, sems.at[0])
    fetch.start()
    nrow, deep, _ = outs[0].shape
    half = keep_ref.shape[1]
    depth = deep - 16
    ncol = half // depth
    across = here_ref[1]
    totals = []
    for r in range(nrow):
        extra = got_ref[r, half : half + 16]
        totals.append([sums_ref[r, n : n + 1] + pieces_sum(extra, n) for n in range(2)])
    fetch.wait()
    for (s, first), out in zip(gather_moves(nrow), outs):
        c = lax.rem(across + s, ncol)
        at = pl.ds(pl.multiple_of(c * depth, depth), depth)
        for k in range(out.shape[0]):
            r = first + k
            out[k, :depth] = (keep_ref[r, at].astype(F32) + got_ref[r, at].astype(F32)).astype(BF16)
            put_pieces(out, (k,), depth, totals[r])


def across_kernel(here_ref, *refs):
    moves = gather_moves(refs[0].shape[0])
    ins, outs = refs[: len(moves)], refs[len(moves) : 2 * len(moves) - 1]
    total_ref, extra_ref = refs[2 * len(moves) - 1 :]
    nrow, deep, _ = ins[0].shape
    depth = deep - 16
    along = here_ref[2]
    for r in range(nrow):
        ends = [ins[0][r], ins[1][r], ins[3 + 2 * r // nrow][r % (nrow // 2)], ins[2][r]]
        total_ref[r] = balanced([one[:depth].astype(F32) for one in ends])
        for n in range(2):
            extra_ref[r, n : n + 1] = balanced([pieces_sum(one[depth:deep], n) for one in ends])
    for s, out in enumerate(outs):
        r = lax.rem(along + s, nrow)
        out[:depth] = total_ref[r].astype(BF16)
        put_pieces(out, (), depth, [extra_ref[r, n : n + 1] for n in range(2)])


def roll_kernel(here_ref, *refs):
    ins, (x_ref, pull_ref, reward_ref) = refs[:-3], refs[-3:]
    depth, deep = x_ref.shape[0], ins[0].shape[0]
    total = balanced([one[:depth].astype(F32) for one in ins])
    sums = [balanced([pieces_sum(one[depth:deep], n) for one in ins]) for n in range(2)]
    reward_ref[...] = (-sums[1] / sums[0])[0]
    pull_ref[...] = sums[0] * x_ref[...].astype(F32) - total


def expert_kernel(got_ref, y_ref, b_ref, pull_ref):
    nz, ny, _, cols = got_ref.shape
    for q in range(ny):
        total = got_ref[0, q].astype(F32)
        for k in range(1, nz):
            total = total + got_ref[k, q].astype(F32)
        at = slice(q * cols, (q + 1) * cols)
        pull_ref[:, at] = b_ref[:, at] * y_ref[:, at].astype(F32) - total


def call(body, outs, scratch, *args, smem=0, far=(), far_out=(), sems=0, limit=None):
    spec = pl.BlockSpec(memory_space=pltpu.VMEM)
    scalar = pl.BlockSpec(memory_space=pltpu.SMEM)
    away = pl.BlockSpec(memory_space=pltpu.HBM)
    ins = [scalar if n < smem else away if n in far else spec for n in range(len(args))]
    args = [pltpu.with_memory_space_constraint(a, pltpu.HBM) if n in far else a for n, a in enumerate(args)]
    scratches = [pltpu.VMEM(s, t) for s, t in scratch]
    if sems:
        scratches.append(pltpu.SemaphoreType.DMA((sems,)))
    return pl.pallas_call(
        body,
        out_shape=[pltpu.HBM(s, t) if n in far_out else jax.ShapeDtypeStruct(s, t) for n, (s, t) in enumerate(outs)],
        in_specs=ins,
        out_specs=[away if n in far_out else spec for n in range(len(outs))],
        scratch_shapes=scratches,
        compiler_params=pltpu.CompilerParams(vmem_limit_bytes=limit),
    )(*args)


def exchanged(x, axes):
    return lax.all_to_all(x, axes, split_axis=0, concat_axis=0, tiled=True)


def as_lines(v, lines):
    count = v.shape[0] // LANES
    return jnp.pad(v.reshape(count, LANES), ((0, lines - count), (0, 0)))


def swapped(x):
    return lax.ppermute(x, "core", [(0, 1), (1, 0)])


def shifted(x, axis, by):
    n = lax.axis_size(axis)
    return lax.ppermute(x, axis, [(i, (i + by) % n) for i in range(n)])


def shards(roll_embed, expert_embed, roll_weight, expert_weight):
    nz, ny, nx, nk = (lax.axis_size(a) for a in ("z", "y", "x", "core"))
    depth, width = roll_embed.shape
    thin, wide = expert_embed.shape
    emb = thin * nz * ny
    cols = wide // ny
    rows = width * ny
    scale = 2.0 * LOG2E / (emb * BLUR)
    grid = (ny, nx, depth, width)
    quarter = lax.axis_index("y")
    here = jnp.stack([lax.axis_index(a).astype(jnp.int32) for a in ("core", "x", "y")])

    x_line = [roll_embed] + [shifted(roll_embed, "y", s) for s in range(1, ny)]
    y_blocks = jnp.moveaxis(expert_embed.reshape(thin, ny, cols), 1, 0)
    y_send = jnp.broadcast_to(y_blocks[None], (nz, ny, thin, cols)).reshape(nz * ny, thin, cols)
    y_all = exchanged(y_send, ("z", "y"))
    y_all = y_all.reshape(emb, cols)
    middle = ny // 2
    x_line = jnp.stack(x_line)
    behind, ahead = shifted(x_line, "x", 1), shifted(x_line, "x", -1)
    x_own = [x_line, behind, ahead, shifted(behind[:middle], "x", 1), shifted(ahead[middle:], "x", -1)]
    x_other = [swapped(x) for x in x_own]

    wtiles = width // LANES
    f_lines = padded(rows // LANES + wtiles, 8)
    g_lines = padded(cols // LANES, 8)
    la_own = as_lines(log2_of(roll_weight), 8)
    lb = as_lines(log2_of(lax.dynamic_slice_in_dim(expert_weight, quarter * cols, cols, 0)), g_lines)
    crowd = ny * nx * nk

    column = ((cols, LANES), F32)
    f_shape, g_shape = (crowd, f_lines, LANES), (nz, g_lines, LANES)
    ins = (here, *x_own, *x_other, y_all, la_own)
    d, sqx, sqy, out, x_all = call(
        functools.partial(setup_kernel, scale, grid),
        [((cols, rows), F32), ((f_lines, LANES), F32), ((g_lines, LANES), F32), (f_shape, F32),
         ((emb, rows), BF16)],
        [((emb, rows), BF16), ((emb, cols), BF16), column, ((f_lines, LANES), F32)],
        *ins, smem=1, far=range(1, 12), far_out=(4,), sems=2 * nx * ny + 2, limit=24 << 20)
    out, lb = lax.optimization_barrier((out, lb))
    la = None
    for step in range(ITERS):
        if step:
            (out,) = call(row_kernel, [(f_shape, F32)], [column, ((f_lines, LANES), F32)],
                          got, lb, d, limit=12 << 20)
        got = exchanged(out, ("y", "x", "core"))
        if step == 0:
            firsts = got.reshape(ny, nx * nk, f_lines, LANES)[:, 0, rows // LANES : rows // LANES + wtiles]
            la = jnp.pad(firsts.reshape(rows // LANES, LANES), ((0, f_lines - rows // LANES), (0, 0)))
        f, out = call(column_kernel, [((f_lines, LANES), F32), (g_shape, F32)],
                      [column, ((g_lines, LANES), F32)], got, la, d, limit=12 << 20)
        got = exchanged(out, ("z",))

    half = nx * depth
    keep, send, sums, xsum = call(
        functools.partial(plan_kernel, scale, emb, grid),
        [((ny, half, width), BF16), ((ny, half + 16, width), BF16), ((ny, 8, width), F32), ((emb, cols), BF16)],
        [((ny, half, width), BF16), ((emb, cols), BF16), column, column, ((cols, rows), BF16), ((emb, cols), BF16),
         ((emb, cols), BF16), ((emb, rows), BF16), ((2, f_lines, LANES), F32)],
        here, got, lb, f, sqx, sqy, d, y_all, x_all, smem=1, far=(7, 8), far_out=(0, 3), sems=4, limit=32 << 20)
    xsum_got = exchanged(xsum.reshape(nz * ny, thin, cols), ("z", "y"))
    line = ((ny, depth + 16, width), BF16)
    short = ((middle, depth + 16, width), BF16)
    own, one, three, two, other_two = call(
        pair_kernel, [line] * 3 + [short] * 2, [((ny, half, width), BF16)], here, keep, sums, swapped(send),
        smem=1, far=(1,), sems=1, limit=16 << 20)
    two, other_two = shifted(two, "x", 1), shifted(other_two, "x", -1)
    lines = [own, shifted(one, "x", 1), shifted(three, "x", -1), shifted(two, "x", 1), shifted(other_two, "x", -1)]
    ends = call(across_kernel, [(line[0][1:], BF16)] * ny, [((ny, depth, width), F32), ((ny, 8, width), F32)],
                here, *lines, smem=1, limit=16 << 20)
    ends = [ends[0]] + [shifted(ends[s], "y", s) for s in range(1, ny)]
    roll_pull, reward = call(roll_kernel, [((depth, width), F32), ((width,), F32)], [],
                             here, *ends, roll_embed, smem=1, limit=8 << 20)
    (expert_pull,) = call(expert_kernel, [((thin, wide), F32)], [],
                          xsum_got.reshape(nz, ny, thin, cols), expert_embed, expert_weight.reshape(1, wide),
                          limit=8 << 20)
    return (reward, roll_pull, expert_pull)


def solution(mesh):
    z, y = 8, 4
    torus = Mesh(mesh.devices.reshape(z, y, 4, 2), ("z", "y", "x", "core"))
    row, col = ("z", "y"), ("x", "core")

    return jax.shard_map(
        shards,
        mesh=torus,
        in_specs=(P(col, row), P(row, col), P(row), P(col)),
        out_specs=(P(row), P(col, row), P(row, col)),
        check_vma=False,
    )
```

```python
import functools
import math

import jax
import jax.numpy as jnp
from jax import lax
from jax.experimental import pallas as pl
from jax.experimental.pallas import tpu as pltpu
from jax.sharding import Mesh
from jax.sharding import PartitionSpec as P

ITERS = 3
BLUR = 0.05
LOG2E = 1.0 / math.log(2.0)
F32 = jnp.float32
BF16 = jnp.bfloat16
LANES = 128
STEP = 64


def cdiv(a, b):
    return -(-a // b)


def padded(n, m):
    return cdiv(n, m) * m


def log2_of(x):
    return jnp.log(x) * LOG2E


def merged(parts):
    high = jnp.max(parts, axis=0)
    return high + log2_of(jnp.sum(jnp.exp2(parts - high[None]), axis=0))


def to_column(lines, column_ref, tiles):
    for t in range(tiles):
        wide = jnp.broadcast_to(lines[t : t + 1, :], (LANES, LANES))
        column_ref[t * LANES : (t + 1) * LANES, :] = wide.T


def row_sweep(d_ref, column_ref, lines_ref):
    cols = d_ref.shape[0]
    chunks = cols // STEP
    tiles = d_ref.shape[1] // LANES

    def one(t, carry):
        lanes = pl.ds(pl.multiple_of(t * LANES, LANES), LANES)

        def score(c):
            at = slice(c * STEP, (c + 1) * STEP)
            return column_ref[at, :] + d_ref[at, lanes]

        top = score(0)
        for c in range(1, chunks):
            top = jnp.maximum(top, score(c))
        top = jnp.max(top, axis=0, keepdims=True)
        total = jnp.exp2(score(0) - top)
        for c in range(1, chunks):
            total = total + jnp.exp2(score(c) - top)
        total = jnp.sum(total, axis=0, keepdims=True)
        lines_ref[pl.ds(t, 1), :] = top + log2_of(total)
        return carry

    lax.fori_loop(0, tiles, one, 0, unroll=3)


def column_sweep(d_ref, lines, column_ref):
    cols = d_ref.shape[0]
    tiles = d_ref.shape[1] // LANES

    def one(c, carry):
        at = pl.ds(pl.multiple_of(c * STEP, STEP), STEP)

        def score(t):
            return lines[t : t + 1, :] + d_ref[at, t * LANES : (t + 1) * LANES]

        top = score(0)
        for t in range(1, tiles):
            top = jnp.maximum(top, score(t))
        top = jnp.max(top, axis=1, keepdims=True)
        total = jnp.exp2(score(0) - top)
        for t in range(1, tiles):
            total = total + jnp.exp2(score(t) - top)
        total = jnp.sum(total, axis=1, keepdims=True)
        column_ref[at, :] = jnp.broadcast_to(top + log2_of(total), (STEP, LANES))
        return carry

    lax.fori_loop(0, cols // STEP, one, 0, unroll=4)


def from_column(column_ref, lines_ref, tiles):
    for t in range(tiles):
        square = column_ref[t * LANES : (t + 1) * LANES, :].T
        lines_ref[t : t + 1, :] = square[0:1, :]


def gather_moves(nrow):
    return ((0, 0), (1, 0), (3, 0), (2, 0), (2, nrow // 2))


def setup_kernel(scale, grid, here_ref, *refs):
    nrow, ncol, depth, width = grid
    moves = gather_moves(nrow)
    own_refs, other_refs = refs[: len(moves)], refs[len(moves) : 2 * len(moves)]
    y_own, y_other, a_ref, b_ref, d_ref, sqx_ref, sqy_ref, out_ref, lb_ref, x_hbm, y_hbm = refs[2 * len(moves) :][:11]
    x_ref, y_ref, column_ref, lines_ref, sems = refs[2 * len(moves) + 11 :]
    part_cols = y_own.shape[1]
    core, across, along = here_ref[0], here_ref[1], here_ref[2]
    fetches = []
    for n, (side, ref) in enumerate(((core, y_own), (1 - core, y_other))):
        lanes = pl.ds(pl.multiple_of(side * part_cols, LANES), part_cols)
        fetches.append(pltpu.make_async_copy(ref, y_ref.at[:, lanes], sems.at[n]))
        fetches[-1].start()
    copies, n = [], 2
    for side, group in ((core, own_refs), (1 - core, other_refs)):
        for (sx, first), ref in zip(moves, group):
            c = lax.rem(across - sx + ncol, ncol)
            at = pl.multiple_of((2 * c + side) * depth, depth)
            for k in range(ref.shape[0]):
                r = lax.rem(along - (first + k) + nrow, nrow)
                lanes = pl.multiple_of(r * width, LANES)
                copy = pltpu.make_async_copy(
                    ref.at[k], x_ref.at[pl.ds(at, depth), pl.ds(lanes, width)], sems.at[n])
                copy.start()
                copies.append(copy)
                n += 1
    for fetch in fetches:
        fetch.wait()
    store_y = pltpu.make_async_copy(y_ref, y_hbm, sems.at[n + 1])
    store_y.start()
    ctiles = y_ref.shape[1] // LANES
    lines_ref[...] = jnp.zeros_like(lines_ref)
    for t in range(ctiles):
        part = y_ref[:, t * LANES : (t + 1) * LANES].astype(F32)
        lines_ref[t : t + 1, :] = jnp.sum(part * part, axis=0, keepdims=True)
    to_column(lines_ref[...], column_ref, ctiles)
    sqy_ref[...] = lines_ref[: sqy_ref.shape[0], :]
    column_ref[...] = column_ref[...] * (-0.5 * scale)
    for copy in copies:
        copy.wait()
    rows = d_ref.shape[1]
    base = core * rows
    mine = x_ref.at[:, pl.ds(pl.multiple_of(base, LANES), rows)]
    store_x = pltpu.make_async_copy(mine, x_hbm, sems.at[n])
    store_x.start()
    tiles = rows // LANES
    sqx_ref[...] = jnp.zeros_like(sqx_ref)
    for t in range(tiles):
        part = x_ref[:, pl.ds(pl.multiple_of(base + t * LANES, LANES), LANES)].astype(F32)
        sqx_ref[t : t + 1, :] = jnp.sum(part * part, axis=0, keepdims=True)
    for r in range(rows // width):
        cross = lax.dot_general(
            y_ref[...], x_ref[:, pl.ds(pl.multiple_of(base + r * width, LANES), width)],
            (((0,), (0,)), ((), ())), preferred_element_type=F32)
        d_ref[:, r * width : (r + 1) * width] = cross * scale
    lines_ref[...] = jnp.zeros_like(lines_ref)
    row_sweep(d_ref, column_ref, lines_ref)
    wtiles = width // LANES
    lines_ref[tiles : tiles + wtiles, :] = log2_of(a_ref[...])
    share = b_ref.shape[0] // nrow
    mine = b_ref[0:share, :]
    for q in range(1, nrow):
        mine = jnp.where(along == q, b_ref[q * share : (q + 1) * share, :], mine)
    lb_ref[...] = log2_of(mine)
    out_ref[...] = jnp.broadcast_to(lines_ref[...][None], out_ref.shape)
    store_x.wait()
    store_y.wait()


def row_kernel(parts_ref, lb_ref, d_ref, out_ref, column_ref, lines_ref):
    ctiles = d_ref.shape[0] // LANES
    g = lb_ref[...] - merged(parts_ref[...])
    to_column(g, column_ref, ctiles)
    lines_ref[...] = jnp.zeros_like(lines_ref)
    row_sweep(d_ref, column_ref, lines_ref)
    out_ref[...] = jnp.broadcast_to(lines_ref[...][None], out_ref.shape)


def first_row_kernel(parts_ref, d_ref, out_ref, lb_ref, column_ref, lines_ref):
    ctiles = d_ref.shape[0] // LANES
    used = lb_ref.shape[0]
    lb_ref[...] = jnp.ones_like(lb_ref)
    for k in range(2):
        lb_ref[k * ctiles // 2 : (k + 1) * ctiles // 2, :] = parts_ref[k, used : used + ctiles // 2, :]
    g = lb_ref[...] - merged(parts_ref[:, :used, :])
    to_column(g, column_ref, ctiles)
    lines_ref[...] = jnp.zeros_like(lines_ref)
    row_sweep(d_ref, column_ref, lines_ref)
    out_ref[...] = jnp.broadcast_to(lines_ref[...][None], out_ref.shape)


def column_kernel(parts_ref, la_ref, d_ref, f_ref, out_ref, column_ref, lines_ref):
    ctiles = d_ref.shape[0] // LANES
    f = la_ref[...] - merged(parts_ref[...])
    f_ref[...] = f
    column_sweep(d_ref, f, column_ref)
    lines_ref[...] = jnp.zeros_like(lines_ref)
    from_column(column_ref, lines_ref, ctiles)
    out_ref[...] = jnp.broadcast_to(lines_ref[...][None], out_ref.shape)


def first_column_kernel(nx, here_ref, parts_ref, lb_ref, d_ref, la_ref, out_ref, column_ref, lines_ref):
    core = here_ref[0]
    ctiles, tiles = d_ref.shape[0] // LANES, d_ref.shape[1] // LANES
    few = parts_ref.shape[0] // nx // 2
    lines = tiles // few
    la_ref[...] = jnp.zeros_like(la_ref)
    for h in range(few):
        la_ref[h * lines : (h + 1) * lines, :] = parts_ref[(core * few + h) * nx, tiles : tiles + lines, :]
    f = la_ref[...] - merged(parts_ref[:, : la_ref.shape[0], :])
    column_sweep(d_ref, f, column_ref)
    lines_ref[...] = jnp.zeros_like(lines_ref)
    from_column(column_ref, lines_ref, ctiles)
    used = lines_ref.shape[0] // 2
    lines_ref[used : used + lb_ref.shape[0], :] = lb_ref[...]
    out_ref[...] = jnp.broadcast_to(lines_ref[...][None], out_ref.shape)


def three_pieces(v):
    high = v.astype(BF16)
    rest = v - high.astype(F32)
    mid = rest.astype(BF16)
    low = (rest - mid.astype(F32)).astype(BF16)
    return high, mid, low


def put_pieces(block_ref, at, row, values):
    block_ref[at + (slice(row, row + 16),)] = jnp.zeros((16, block_ref.shape[-1]), BF16)
    for n, v in enumerate(values):
        for m, piece in enumerate(three_pieces(v)):
            block_ref[at + (slice(row + 3 * n + m, row + 3 * n + m + 1),)] = piece


def pieces_sum(block, n):
    one, two, three = (block[3 * n + m : 3 * n + m + 1].astype(F32) for m in range(3))
    return one + two + three


def balanced(values):
    while len(values) > 1:
        half = len(values) // 2
        values = [values[k] + values[k + half] for k in range(half)]
    return values[0]


def plan_kernel(scale, emb, grid, here_ref, parts_ref, lb_ref, f_ref, sqx_ref, sqy_ref, d_ref, y_hbm, x_hbm,
                keep_ref, send_ref, sums_ref, xkeep_ref, xsend_ref, column_ref, square_ref, plan_ref, y_ref, ys_ref, x_ref,
                lines_ref, sems):
    core = here_ref[0]
    nrow, ncol, depth, width = grid
    half = ncol * depth
    cols, rows = d_ref.shape
    ctiles, tiles, chunks = cols // LANES, rows // LANES, cols // STEP
    copies = [pltpu.make_async_copy(y_hbm, y_ref, sems.at[0]), pltpu.make_async_copy(x_hbm, x_ref, sems.at[1])]
    for copy in copies:
        copy.start()
    g = lb_ref[...] - merged(parts_ref[...])
    to_column(g, column_ref, ctiles)
    back = 1.0 / emb
    unit = 2.0 / (emb * scale)
    to_column(sqy_ref[...], square_ref, ctiles)

    def one(t, carry):
        lanes = pl.ds(pl.multiple_of(t * LANES, LANES), LANES)
        f = f_ref[pl.ds(t, 1), :]
        sq = sqx_ref[pl.ds(t, 1), :]
        mass = jnp.zeros((STEP, LANES), F32)
        paid = jnp.zeros((STEP, LANES), F32)
        for c in range(chunks):
            at = slice(c * STEP, (c + 1) * STEP)
            d = d_ref[at, lanes]
            p = jnp.exp2(column_ref[at, :] + d + f)
            plan_ref[at, lanes] = p.astype(BF16)
            mass = mass + p
            paid = paid + p * ((sq + square_ref[at, :]) * back - d * unit)
        lines_ref[0, pl.ds(t, 1), :] = jnp.sum(mass, axis=0, keepdims=True)
        lines_ref[1, pl.ds(t, 1), :] = jnp.sum(paid, axis=0, keepdims=True)
        return carry

    lax.fori_loop(0, tiles, one, 0, unroll=2)
    sums_ref[...] = jnp.zeros_like(sums_ref)
    wtiles = width // LANES
    for r in range(nrow):
        for w in range(wtiles):
            t = r * wtiles + w
            for n in range(2):
                sums_ref[r, n : n + 1, w * LANES : (w + 1) * LANES] = lines_ref[n, t : t + 1, :]
    for copy in copies:
        copy.wait()
    part = cols // 2
    for side, ref in ((core, xkeep_ref), (1 - core, xsend_ref)):
        at = pl.ds(pl.multiple_of(side * part, part), part)
        ref[...] = lax.dot_general(
            x_ref[...], plan_ref[at, :], (((1,), (1,)), ((), ())), preferred_element_type=F32).astype(BF16)
    for c in range(ncol):
        mine = pl.multiple_of((2 * c + core) * depth, depth)
        theirs = pl.multiple_of((2 * c + 1 - core) * depth, depth)
        ys_ref[c * depth : (c + 1) * depth, :] = y_ref[pl.ds(mine, depth), :]
        ys_ref[half + c * depth : half + (c + 1) * depth, :] = y_ref[pl.ds(theirs, depth), :]
    for r in range(nrow):
        part = plan_ref[:, r * width : (r + 1) * width]
        pulled = lax.dot_general(ys_ref[...], part, (((1,), (0,)), ((), ())), preferred_element_type=F32)
        keep_ref[r] = pulled[:half].astype(BF16)
        send_ref[r, :half] = pulled[half:].astype(BF16)
        put_pieces(send_ref, (r,), half, [sums_ref[r, n : n + 1] for n in range(2)])


def pair_kernel(here_ref, keep_ref, sums_ref, got_ref, *refs):
    outs, (full_ref, stats_ref) = refs[:-2], refs[-2:]
    core, across = here_ref[0], here_ref[1]
    part, half = keep_ref.shape[0], keep_ref.shape[1]
    nrow, deep, _ = outs[0].shape
    depth = deep - 16
    ncol = half // depth
    for k in range(part):
        full_ref[core * part + k] = keep_ref[k]
        full_ref[(1 - core) * part + k] = got_ref[k, :half]
        extra = got_ref[k, half : half + 16]
        for n in range(2):
            stats_ref[core * part + k, n : n + 1] = sums_ref[k, n : n + 1]
            stats_ref[(1 - core) * part + k, n : n + 1] = pieces_sum(extra, n)
    for (s, first), out in zip(gather_moves(nrow), outs):
        c = lax.rem(across + s, ncol)
        at = pl.ds(pl.multiple_of(c * depth, depth), depth)
        for k in range(out.shape[0]):
            r = first + k
            out[k, :depth] = full_ref[r, at]
            put_pieces(out, (k,), depth, [stats_ref[r, n : n + 1] for n in range(2)])


def sum_kernel(kept_ref, got_ref, out_ref):
    out_ref[...] = (kept_ref[...].astype(F32) + got_ref[...].astype(F32)).astype(BF16)


def across_kernel(here_ref, *refs):
    moves = gather_moves(refs[0].shape[0])
    ins, outs = refs[: len(moves)], refs[len(moves) : 2 * len(moves) - 1]
    total_ref, extra_ref = refs[2 * len(moves) - 1 :]
    nrow, deep, _ = ins[0].shape
    depth = deep - 16
    along = here_ref[2]
    for r in range(nrow):
        ends = [ins[0][r], ins[1][r], ins[3 + 2 * r // nrow][r % (nrow // 2)], ins[2][r]]
        total_ref[r] = balanced([one[:depth].astype(F32) for one in ends])
        for n in range(2):
            extra_ref[r, n : n + 1] = balanced([pieces_sum(one[depth:deep], n) for one in ends])
    for s, out in enumerate(outs):
        r = lax.rem(along + s, nrow)
        out[:depth] = total_ref[r].astype(BF16)
        put_pieces(out, (), depth, [extra_ref[r, n : n + 1] for n in range(2)])


def roll_kernel(here_ref, *refs):
    ins, (x_ref, pull_ref, reward_ref) = refs[:-3], refs[-3:]
    depth, deep = x_ref.shape[0], ins[0].shape[0]
    total = balanced([one[:depth].astype(F32) for one in ins])
    sums = [balanced([pieces_sum(one[depth:deep], n) for one in ins]) for n in range(2)]
    reward_ref[...] = (-sums[1] / sums[0])[0]
    pull_ref[...] = sums[0] * x_ref[...].astype(F32) - total


def expert_kernel(got_ref, y_ref, b_ref, pull_ref):
    nz, ny, _, cols = got_ref.shape
    for q in range(ny):
        total = got_ref[0, q].astype(F32)
        for k in range(1, nz):
            total = total + got_ref[k, q].astype(F32)
        at = slice(q * cols, (q + 1) * cols)
        pull_ref[:, at] = b_ref[:, at] * y_ref[:, at].astype(F32) - total


def call(body, outs, scratch, *args, smem=0, far=(), far_out=(), sems=0, limit=None):
    spec = pl.BlockSpec(memory_space=pltpu.VMEM)
    scalar = pl.BlockSpec(memory_space=pltpu.SMEM)
    away = pl.BlockSpec(memory_space=pltpu.HBM)
    ins = [scalar if n < smem else away if n in far else spec for n in range(len(args))]
    args = [pltpu.with_memory_space_constraint(a, pltpu.HBM) if n in far else a for n, a in enumerate(args)]
    scratches = [pltpu.VMEM(s, t) for s, t in scratch]
    if sems:
        scratches.append(pltpu.SemaphoreType.DMA((sems,)))
    return pl.pallas_call(
        body,
        out_shape=[pltpu.HBM(s, t) if n in far_out else jax.ShapeDtypeStruct(s, t) for n, (s, t) in enumerate(outs)],
        in_specs=ins,
        out_specs=[away if n in far_out else spec for n in range(len(outs))],
        scratch_shapes=scratches,
        compiler_params=pltpu.CompilerParams(vmem_limit_bytes=limit),
    )(*args)


def exchanged(x, axes):
    return lax.all_to_all(x, axes, split_axis=0, concat_axis=0, tiled=True)


def swapped(x):
    return lax.ppermute(x, "core", [(0, 1), (1, 0)])


def shifted(x, axis, by):
    n = lax.axis_size(axis)
    return lax.ppermute(x, axis, [(i, (i + by) % n) for i in range(n)])


def shards(roll_embed, expert_embed, roll_weight, expert_weight):
    nz, ny, nx, nk = (lax.axis_size(a) for a in ("z", "y", "x", "core"))
    depth, width = roll_embed.shape
    thin, wide = expert_embed.shape
    emb = thin * nz * ny
    part = wide // ny
    cols = part * nk
    rows = width * ny // nk
    scale = 2.0 * LOG2E / (emb * BLUR)
    grid = (ny // nk, nx, depth, width)
    here = jnp.stack([lax.axis_index(a).astype(jnp.int32) for a in ("core", "x", "y")])

    x_line = [roll_embed] + [shifted(roll_embed, "y", s) for s in range(1, ny)]
    y_blocks = jnp.moveaxis(expert_embed.reshape(thin, ny, part), 1, 0)
    y_send = jnp.broadcast_to(y_blocks[None], (nz, ny, thin, part)).reshape(nz * ny, thin, part)
    y_all = exchanged(y_send, ("z", "y"))
    y_own = y_all.reshape(emb, part)
    y_other = swapped(y_own)
    middle = ny // 2
    x_line = jnp.stack(x_line)
    behind, ahead = shifted(x_line, "x", 1), shifted(x_line, "x", -1)
    halves = [shifted(behind[:middle], "x", 1), shifted(ahead[middle:], "x", -1)]
    x_own = [x_line, behind, ahead, *halves]
    x_other = [swapped(x) for x in x_own[:3]]
    x_other += [swapped(x) for x in halves]

    wtiles = width // LANES
    f_lines = padded(rows // LANES + wtiles, 8)
    g_lines = padded(cols // LANES, 8)
    a_lines = roll_weight.reshape(-1, LANES)
    b_lines = expert_weight.reshape(-1, LANES)

    column = ((cols, LANES), F32)
    crowd = ny * nx
    t_lines = padded(rows // LANES, 8)
    f_shape, g_shape = (crowd, t_lines, LANES), (nz * nk, g_lines, LANES)
    ins = (here, *x_own, *x_other, y_own, y_other, a_lines, b_lines)
    d, sqx, sqy, out, lb_own, x_all, y_all = call(
        functools.partial(setup_kernel, scale, (ny, nx, depth, width)),
        [((cols, rows), F32), ((t_lines, LANES), F32), ((g_lines, LANES), F32), ((crowd, f_lines, LANES), F32),
         ((part // LANES, LANES), F32),
         ((emb, rows), BF16), ((emb, cols), BF16)],
        [((emb, rows * nk), BF16), ((emb, cols), BF16), column, ((f_lines, LANES), F32)],
        *ins, smem=1, far=range(1, 13), far_out=(5, 6), sems=2 * nx * ny + 4, limit=24 << 20)
    g_column = [column, ((g_lines, LANES), F32)]
    got = exchanged(out, ("y", "x"))
    la, out = call(functools.partial(first_column_kernel, nx),
                   [((t_lines, LANES), F32), ((nz * nk, 2 * g_lines, LANES), F32)],
                   [column, ((2 * g_lines, LANES), F32)], here, got, lb_own, d, smem=1, limit=12 << 20)
    got = exchanged(out, ("z", "core"))
    out, lb = call(first_row_kernel, [(f_shape, F32), ((g_lines, LANES), F32)], [column, ((t_lines, LANES), F32)],
                   got, d, limit=12 << 20)
    for step in range(1, ITERS):
        if step > 1:
            (out,) = call(row_kernel, [(f_shape, F32)], [column, ((t_lines, LANES), F32)], got, lb, d, limit=12 << 20)
        got = exchanged(out, ("y", "x"))
        f, out = call(column_kernel, [((t_lines, LANES), F32), (g_shape, F32)], g_column, got, la, d, limit=12 << 20)
        got = exchanged(out, ("z", "core"))

    half = nx * depth
    few = ny // nk
    keep, send, sums, xkeep, xsend = call(
        functools.partial(plan_kernel, scale, emb, grid),
        [((few, half, width), BF16), ((few, half + 16, width), BF16), ((few, 8, width), F32), ((emb, part), BF16),
         ((emb, part), BF16)],
        [column, column, ((cols, rows), BF16), ((emb, cols), BF16),
         ((emb, cols), BF16), ((emb, rows), BF16), ((2, t_lines, LANES), F32)],
        here, got, lb, f, sqx, sqy, d, y_all, x_all, smem=1, far=(7, 8), sems=2, limit=32 << 20)
    line = ((ny, depth + 16, width), BF16)
    short = ((middle, depth + 16, width), BF16)
    pull_got, xsum_got = swapped(send), swapped(xsend)
    own, one, three, two, other_two = call(
        pair_kernel, [line] * 3 + [short] * 2, [((ny, half, width), BF16), ((ny, 8, width), F32)],
        here, keep, sums, pull_got, smem=1, limit=16 << 20)
    (xsum,) = call(sum_kernel, [((emb, part), BF16)], [], xkeep, xsum_got, limit=8 << 20)
    xsum_got = exchanged(xsum.reshape(nz * ny, thin, part), ("z", "y"))
    two, other_two = shifted(two, "x", 1), shifted(other_two, "x", -1)
    one, three = shifted(one, "x", 1), shifted(three, "x", -1)
    lines = [own, one, three, shifted(two, "x", 1), shifted(other_two, "x", -1)]
    ends = call(across_kernel, [(line[0][1:], BF16)] * ny, [((ny, depth, width), F32), ((ny, 8, width), F32)],
                here, *lines, smem=1, limit=16 << 20)
    ends = [ends[0]] + [shifted(ends[s], "y", s) for s in range(1, ny)]
    roll_pull, reward = call(roll_kernel, [((depth, width), F32), ((width,), F32)], [],
                             here, *ends, roll_embed, smem=1, limit=8 << 20)
    (expert_pull,) = call(expert_kernel, [((thin, wide), F32)], [],
                          xsum_got.reshape(nz, ny, thin, part), expert_embed, expert_weight.reshape(1, wide),
                          limit=8 << 20)
    return (reward, roll_pull, expert_pull)


def solution(mesh):
    z, y = 8, 4
    torus = Mesh(mesh.devices.reshape(z, y, 4, 2), ("z", "y", "x", "core"))
    row, col = ("z", "y"), ("x", "core")

    return jax.shard_map(
        shards,
        mesh=torus,
        in_specs=(P(col, row), P(row, col), P(row), P(col)),
        out_specs=(P(row), P(col, row), P(row, col)),
        check_vma=False,
    )
```
